8 devices in a mesh: dp: 1 (over z), tp: 8 (over y, x, core).
Axes of the slice: x: 2, y: 2, z: 1, core: 2. Of those that a mesh axis runs over, the one named last changes fastest.
Arguments:
- x_in: bfloat16 [2, 2048, 1152], P('dp', 'tp')
- y_text: bfloat16 [2, 120, 1152], P('dp', 'tp')
- t_emb: bfloat16 [2, 6912], P('dp')
- text_len: int32 [2], P('dp')
- mod_table: bfloat16 [6, 1152], replicated
- w_qkv: bfloat16 [1152, 16, 216], P(None, 'tp')
- b_qkv: bfloat16 [16, 216], P('tp')
- w_o: bfloat16 [16, 72, 1152], P('tp')
- b_o: bfloat16 [1152], replicated
- w_q: bfloat16 [1152, 16, 72], P(None, 'tp')
- b_q: bfloat16 [16, 72], P('tp')
- w_kv: bfloat16 [1152, 16, 144], P(None, 'tp')
- b_kv: bfloat16 [16, 144], P('tp')
- w_co: bfloat16 [16, 72, 1152], P('tp')
- b_co: bfloat16 [1152], replicated
- w_1: bfloat16 [1152, 4608], P(None, 'tp')
- b_1: bfloat16 [4608], P('tp')
- w_2: bfloat16 [4608, 1152], P('tp')
- b_2: bfloat16 [1152], replicated
- g_out: bfloat16 [2, 2048, 1152], P('dp', 'tp')
Outputs:
- output 1: bfloat16 [2, 2048, 1152], P('dp', 'tp')
- output 2: bfloat16 [2, 2048, 1152], P('dp', 'tp')
- output 3: bfloat16 [2, 120, 1152], P('dp', 'tp')
- output 4: float32 [6, 1152], P('dp')
- output 5: bfloat16 [1152, 16, 216], P('dp', 'tp')
- output 6: bfloat16 [16, 216], P(('dp', 'tp'))
- output 7: bfloat16 [16, 72, 1152], P(('dp', 'tp'))
- output 8: bfloat16 [1152], P('dp')
- output 9: bfloat16 [1152, 16, 72], P('dp', 'tp')
- output 10: bfloat16 [16, 72], P(('dp', 'tp'))
- output 11: bfloat16 [1152, 16, 144], P('dp', 'tp')
- output 12: bfloat16 [16, 144], P(('dp', 'tp'))
- output 13: bfloat16 [16, 72, 1152], P(('dp', 'tp'))
- output 14: bfloat16 [1152], P('dp')
- output 15: bfloat16 [1152, 4608], P('dp', 'tp')
- output 16: bfloat16 [4608], P(('dp', 'tp'))
- output 17: bfloat16 [4608, 1152], P(('dp', 'tp'))
- output 18: bfloat16 [1152], P('dp')
All inputs are finite; a program needn't handle non-finite values.
Results may differ from the reference program's by a relative error of at most 0.0195586.
Values are sent between devices in bfloat16 or wider.
A program may use at most 1 GiB of HBM per device.

```python
import jax
import jax.numpy as jnp
from jax import lax

BATCH_SIZE = 2
IMG_TOKENS = 2048
TEXT_SLOTS = 120
TEXT_LEN = 120
WIDTH = 1152
NUM_HEADS = 16
HEAD_DIM = 72
FFN_DIM = 4608
LN_EPS = 1e-6


def setup_inputs(seed: int = 0, part: int = 0) -> dict:
    part_keys = jax.random.split(jax.random.fold_in(jax.random.key(seed), part), 5)
    weight_keys = jax.random.split(jax.random.key(seed + 1), 15)
    width_scale = WIDTH ** -0.5

    def draw_normal(rng_key, shape, scale):
        return (scale * jax.random.normal(rng_key, shape, jnp.float32)).astype(jnp.bfloat16)

    lengths = jax.random.randint(part_keys[3], (BATCH_SIZE,), 1, TEXT_LEN + 1)
    lengths = jnp.where(jnp.arange(BATCH_SIZE) == 0, TEXT_LEN, lengths).astype(jnp.int32)
    return {
        'x_in': draw_normal(part_keys[0], (BATCH_SIZE, IMG_TOKENS, WIDTH), 1.0),
        'y_text': draw_normal(part_keys[1], (BATCH_SIZE, TEXT_SLOTS, WIDTH), 1.0),
        't_emb': draw_normal(part_keys[2], (BATCH_SIZE, 6 * WIDTH), 0.3),
        'text_len': lengths,
        'mod_table': draw_normal(weight_keys[0], (6, WIDTH), 0.3),
        'w_qkv': draw_normal(weight_keys[1], (WIDTH, NUM_HEADS, 3 * HEAD_DIM), width_scale),
        'b_qkv': draw_normal(weight_keys[2], (NUM_HEADS, 3 * HEAD_DIM), 0.2),
        'w_o': draw_normal(weight_keys[3], (NUM_HEADS, HEAD_DIM, WIDTH), width_scale),
        'b_o': draw_normal(weight_keys[4], (WIDTH,), 0.2),
        'w_q': draw_normal(weight_keys[5], (WIDTH, NUM_HEADS, HEAD_DIM), width_scale),
        'b_q': draw_normal(weight_keys[6], (NUM_HEADS, HEAD_DIM), 0.2),
        'w_kv': draw_normal(weight_keys[7], (WIDTH, NUM_HEADS, 2 * HEAD_DIM), width_scale),
        'b_kv': draw_normal(weight_keys[8], (NUM_HEADS, 2 * HEAD_DIM), 0.2),
        'w_co': draw_normal(weight_keys[9], (NUM_HEADS, HEAD_DIM, WIDTH), 2.0 * width_scale),
        'b_co': draw_normal(weight_keys[10], (WIDTH,), 0.2),
        'w_1': draw_normal(weight_keys[11], (WIDTH, FFN_DIM), width_scale),
        'b_1': draw_normal(weight_keys[12], (FFN_DIM,), 0.2),
        'w_2': draw_normal(weight_keys[13], (FFN_DIM, WIDTH), FFN_DIM ** -0.5),
        'b_2': draw_normal(weight_keys[14], (WIDTH,), 0.2),
        'g_out': draw_normal(part_keys[4], (BATCH_SIZE, IMG_TOKENS, WIDTH), 1.0),
    }


def as_bf16(tensor):
    return tensor.astype(jnp.bfloat16).astype(jnp.float32)


def layer_norm(tensor):
    centered = tensor - jnp.mean(tensor, axis=-1, keepdims=True)
    variance = jnp.mean(centered * centered, axis=-1, keepdims=True)
    return centered * lax.rsqrt(variance + LN_EPS)


def split_heads(tensor):
    batch, length = tensor.shape[0], tensor.shape[1]
    return tensor.transpose(0, 2, 1, 3).reshape(batch * NUM_HEADS, length, HEAD_DIM)


def merge_heads(tensor, batch):
    length = tensor.shape[1]
    return tensor.reshape(batch, NUM_HEADS, length, HEAD_DIM).transpose(0, 2, 1, 3)


def attention(q_heads, k_heads, v_heads, key_ok):
    def one_head(operands):
        q_blk, k_blk, v_blk, ok_row = operands
        scores = jnp.dot(q_blk, k_blk.T, preferred_element_type=jnp.float32) * HEAD_DIM ** -0.5
        scores = jnp.where(ok_row[None, :], scores, -1e30)
        weights = jax.nn.softmax(scores, axis=-1)
        return jnp.dot(weights, v_blk, preferred_element_type=jnp.float32)
    return lax.map(jax.checkpoint(one_head), (q_heads, k_heads, v_heads, key_ok))


def block_forward(x_val, y_val, params, t_val, text_len):
    (mod_table, w_qkv, b_qkv, w_o, b_o, w_q, b_q, w_kv, b_kv, w_co, b_co, w_1, b_1, w_2, b_2) = params
    batch = x_val.shape[0]
    mod_rows = mod_table[None] + t_val.reshape(batch, 6, WIDTH)
    shift1 = mod_rows[:, 0, None, :]
    scale1 = mod_rows[:, 1, None, :]
    gate1 = mod_rows[:, 2, None, :]
    shift2 = mod_rows[:, 3, None, :]
    scale2 = mod_rows[:, 4, None, :]
    gate2 = mod_rows[:, 5, None, :]
    h_one = as_bf16(layer_norm(x_val) * (1.0 + scale1) + shift1)
    qkv_all = as_bf16(jnp.einsum('bnd,dhe->bnhe', h_one, w_qkv) + b_qkv)
    self_ok = jnp.ones((batch * NUM_HEADS, IMG_TOKENS), dtype=jnp.bool_)
    attn_val = attention(split_heads(qkv_all[..., :HEAD_DIM]), split_heads(qkv_all[..., HEAD_DIM:2 * HEAD_DIM]), split_heads(qkv_all[..., 2 * HEAD_DIM:]), self_ok)
    attn_val = as_bf16(merge_heads(attn_val, batch))
    x_one = as_bf16(x_val + gate1 * (jnp.einsum('bnhe,hed->bnd', attn_val, w_o) + b_o))
    q_cross = as_bf16(jnp.einsum('bnd,dhe->bnhe', x_one, w_q) + b_q)
    kv_cross = as_bf16(jnp.einsum('bsd,dhe->bshe', y_val, w_kv) + b_kv)
    slot_ok = jnp.arange(TEXT_SLOTS)[None, :] < text_len[:, None]
    cross_ok = jnp.broadcast_to(slot_ok[:, None, :], (batch, NUM_HEADS, TEXT_SLOTS)).reshape(batch * NUM_HEADS, TEXT_SLOTS)
    cross_val = attention(split_heads(q_cross), split_heads(kv_cross[..., :HEAD_DIM]), split_heads(kv_cross[..., HEAD_DIM:]), cross_ok)
    cross_val = as_bf16(merge_heads(cross_val, batch))
    x_two = as_bf16(x_one + jnp.einsum('bnhe,hed->bnd', cross_val, w_co) + b_co)
    h_two = as_bf16(layer_norm(x_two) * (1.0 + scale2) + shift2)
    hidden = jnp.einsum('bnd,df->bnf', h_two, w_1) + b_1
    gelu_out = as_bf16(jax.nn.gelu(hidden, approximate=True))
    return x_two + gate2 * (jnp.einsum('bnf,fd->bnd', gelu_out, w_2) + b_2)


def reference(x_in, y_text, t_emb, text_len, mod_table, w_qkv, b_qkv, w_o, b_o, w_q, b_q, w_kv, b_kv, w_co, b_co, w_1, b_1, w_2, b_2, g_out):
    params = tuple(weight.astype(jnp.float32) for weight in (mod_table, w_qkv, b_qkv, w_o, b_o, w_q, b_q, w_kv, b_kv, w_co, b_co, w_1, b_1, w_2, b_2))
    t_val = t_emb.astype(jnp.float32)

    def forward(x_val, y_val, param_set):
        return block_forward(x_val, y_val, param_set, t_val, text_len)

    x_out, back = jax.vjp(forward, x_in.astype(jnp.float32), y_text.astype(jnp.float32), params)
    g_x, g_y, g_par = back(g_out.astype(jnp.float32))
    return (x_out.astype(jnp.bfloat16), g_x.astype(jnp.bfloat16), g_y.astype(jnp.bfloat16), g_par[0], g_par[1].astype(jnp.bfloat16), g_par[2].astype(jnp.bfloat16), g_par[3].astype(jnp.bfloat16), g_par[4].astype(jnp.bfloat16), g_par[5].astype(jnp.bfloat16), g_par[6].astype(jnp.bfloat16), g_par[7].astype(jnp.bfloat16), g_par[8].astype(jnp.bfloat16), g_par[9].astype(jnp.bfloat16), g_par[10].astype(jnp.bfloat16), g_par[11].astype(jnp.bfloat16), g_par[12].astype(jnp.bfloat16), g_par[13].astype(jnp.bfloat16), g_par[14].astype(jnp.bfloat16))
```

```python
import functools
import math

import jax
import jax.numpy as jnp
from jax import lax
from jax.experimental import pallas as pl
from jax.experimental.pallas import tpu as pltpu
from jax.sharding import PartitionSpec as P

LN_EPS = 1e-6
MASK_FILL = -1e30
N_DEV = 8
LOG2E = math.log2(math.e)
BF = jnp.bfloat16
F32 = jnp.float32


def product(form, lhs, rhs):
    return jnp.einsum(form, lhs, rhs, preferred_element_type=F32)


def layer_norm(tensor):
    tensor = tensor.astype(F32)
    centered = tensor - jnp.mean(tensor, axis=-1, keepdims=True)
    inv_std = lax.rsqrt(jnp.mean(centered * centered, axis=-1, keepdims=True) + LN_EPS)
    return centered * inv_std, inv_std


def layer_norm_back(normed, inv_std, g_normed):
    mean_g = jnp.mean(g_normed, axis=-1, keepdims=True)
    mean_gn = jnp.mean(g_normed * normed, axis=-1, keepdims=True)
    return inv_std * (g_normed - mean_g - normed * mean_gn)


def gelu_tanh(tensor):
    return jax.nn.gelu(tensor, approximate=True)


def dot00(lhs, rhs):
    return lax.dot_general(lhs, rhs, (((0,), (0,)), ((), ())), preferred_element_type=F32)


def dot10(lhs, rhs):
    return lax.dot_general(lhs, rhs, (((1,), (0,)), ((), ())), preferred_element_type=F32)


def dot11(lhs, rhs):
    return lax.dot_general(lhs, rhs, (((1,), (1,)), ((), ())), preferred_element_type=F32)


def attn_fwd_kernel(scale, blk, qkv_ref, o_ref, lse_ref):
    tokens = o_ref.shape[2]
    factor = scale * LOG2E

    def step(j, carry):
        cols = pl.ds(pl.multiple_of(j * blk, blk), blk)
        s = dot00(qkv_ref[0, 1], qkv_ref[0, 0, :, cols])
        top = jnp.max(s, axis=0, keepdims=True) * factor
        p = jnp.exp2(s * factor - top)
        total = jnp.sum(p, axis=0, keepdims=True)
        o = dot10(qkv_ref[0, 2], p.astype(BF))
        o_ref[0, :, cols] = (o / total).astype(BF)
        lse_ref[0, :, cols] = top + jnp.log2(total)
        return carry

    lax.fori_loop(0, tokens // blk, step, 0)


def attn_fwd(qkv, blk=256):
    heads, _, hd, tokens = qkv.shape
    return pl.pallas_call(
        functools.partial(attn_fwd_kernel, hd ** -0.5, blk),
        grid=(heads,),
        in_specs=[pl.BlockSpec((1, 3, hd, tokens), lambda h: (h, 0, 0, 0))],
        out_specs=[pl.BlockSpec((1, hd, tokens), lambda h: (h, 0, 0)), pl.BlockSpec((1, 1, tokens), lambda h: (h, 0, 0))],
        out_shape=[jax.ShapeDtypeStruct((heads, hd, tokens), BF), jax.ShapeDtypeStruct((heads, 1, tokens), F32)],
        cost_estimate=pl.CostEstimate(flops=4 * heads * hd * tokens * tokens, bytes_accessed=heads * hd * tokens * 8, transcendentals=heads * tokens * tokens),
        compiler_params=pltpu.CompilerParams(vmem_limit_bytes=48 << 20),
        name="attn_fwd",
    )(qkv)


def attn_bwd_kernel(scale, blk, qkv_ref, o_ref, lse_ref, g_ref, d_ref, dk_acc, dv_acc):
    tokens = o_ref.shape[2]
    factor = scale * LOG2E
    dk_acc[...] = jnp.zeros_like(dk_acc)
    dv_acc[...] = jnp.zeros_like(dv_acc)

    def step(j, carry):
        cols = pl.ds(pl.multiple_of(j * blk, blk), blk)
        q = qkv_ref[0, 0, :, cols]
        g = g_ref[0, :, cols]
        delta = jnp.sum(g.astype(F32) * o_ref[0, :, cols].astype(F32), axis=0, keepdims=True)
        s = dot00(qkv_ref[0, 1], q)
        p = jnp.exp2(s * factor - lse_ref[0, :, cols])
        dp = dot00(qkv_ref[0, 2], g)
        ds = (p * (dp - delta)).astype(BF)
        dv_acc[...] += dot11(g, p.astype(BF))
        dk_acc[...] += dot11(q, ds)
        d_ref[0, 0, :, cols] = (dot10(qkv_ref[0, 1], ds) * scale).astype(BF)
        return carry

    lax.fori_loop(0, tokens // blk, step, 0)
    d_ref[0, 1] = (dk_acc[...] * scale).astype(BF)
    d_ref[0, 2] = dv_acc[...].astype(BF)


def attn_bwd(qkv, o, lse, g, blk=256):
    heads, _, hd, tokens = qkv.shape
    row = lambda h: (h, 0, 0)
    return pl.pallas_call(
        functools.partial(attn_bwd_kernel, hd ** -0.5, blk),
        grid=(heads,),
        in_specs=[pl.BlockSpec((1, 3, hd, tokens), lambda h: (h, 0, 0, 0)), pl.BlockSpec((1, hd, tokens), row), pl.BlockSpec((1, 1, tokens), row), pl.BlockSpec((1, hd, tokens), row)],
        out_specs=pl.BlockSpec((1, 3, hd, tokens), lambda h: (h, 0, 0, 0)),
        out_shape=jax.ShapeDtypeStruct((heads, 3, hd, tokens), BF),
        scratch_shapes=[pltpu.VMEM((hd, tokens), F32), pltpu.VMEM((hd, tokens), F32)],
        cost_estimate=pl.CostEstimate(flops=10 * heads * hd * tokens * tokens, bytes_accessed=heads * hd * tokens * 20, transcendentals=heads * tokens * tokens),
        compiler_params=pltpu.CompilerParams(vmem_limit_bytes=48 << 20),
        name="attn_bwd",
    )(qkv, o, lse, g)


def cross_fwd_kernel(scale, len_ref, q_ref, kv_ref, c_ref, p_ref):
    heads, slots = q_ref.shape[1], kv_ref.shape[5]
    blk = q_ref.shape[3]
    count = len_ref[pl.program_id(0)]
    ok = lax.broadcasted_iota(jnp.int32, (slots, blk), 0) < count
    for h in range(heads):
        s = dot00(kv_ref[h // 2, 0, h % 2, 0], q_ref[0, h]) * scale
        s = jnp.where(ok, s, MASK_FILL)
        p = jnp.exp(s - jnp.max(s, axis=0, keepdims=True))
        p = (p / jnp.sum(p, axis=0, keepdims=True)).astype(BF)
        p_ref[0, h] = p
        c_ref[0, h] = dot10(kv_ref[h // 2, 0, h % 2, 1], p).astype(BF)


def cross_specs(hd, blk, slots, per):
    q_spec = pl.BlockSpec((1, per, hd, blk), lambda b, i, n: (b, i, 0, 0))
    kv_spec = pl.BlockSpec((per // 2, 1, 2, 2, hd, slots), lambda b, i, n: (i, b, 0, 0, 0, 0))
    p_spec = pl.BlockSpec((1, per, slots, blk), lambda b, i, n: (b, i, 0, 0))
    return q_spec, kv_spec, p_spec


def cross_fwd(lens, q, kv, per=8):
    batch, heads, hd, blk = q.shape
    slots = kv.shape[5]
    q_spec, kv_spec, p_spec = cross_specs(hd, blk, slots, per)
    return pl.pallas_call(
        functools.partial(cross_fwd_kernel, hd ** -0.5),
        grid_spec=pltpu.PrefetchScalarGridSpec(num_scalar_prefetch=1, grid=(batch, heads // per), in_specs=[q_spec, kv_spec], out_specs=[q_spec, p_spec]),
        out_shape=[jax.ShapeDtypeStruct(q.shape, BF), jax.ShapeDtypeStruct((batch, heads, slots, blk), BF)],
        cost_estimate=pl.CostEstimate(flops=4 * batch * heads * hd * blk * slots * 8, bytes_accessed=batch * heads * blk * (hd * 4 + slots * 2), transcendentals=batch * heads * blk * slots),
        compiler_params=pltpu.CompilerParams(vmem_limit_bytes=32 << 20),
        name="cross_fwd",
    )(lens, q, kv)


def cross_bwd_kernel(scale, len_ref, q_ref, kv_ref, p_ref, g_ref, gq_ref, gkv_ref):
    heads = q_ref.shape[1]
    for h in range(heads):
        k, v = kv_ref[h // 2, 0, h % 2, 0], kv_ref[h // 2, 0, h % 2, 1]
        q, g, p = q_ref[0, h], g_ref[0, h], p_ref[0, h]
        dp = dot00(v, g)
        pf = p.astype(F32)
        delta = jnp.sum(dp * pf, axis=0, keepdims=True)
        ds = (pf * (dp - delta) * scale).astype(BF)
        gq_ref[0, h] = dot10(k, ds).astype(BF)
        gkv_ref[h // 2, 0, h % 2, 0] = dot11(q, ds).astype(BF)
        gkv_ref[h // 2, 0, h % 2, 1] = dot11(g, p).astype(BF)


def cross_bwd(lens, q, kv, prob, g, per=8):
    batch, heads, hd, blk = q.shape
    slots = kv.shape[5]
    q_spec, kv_spec, p_spec = cross_specs(hd, blk, slots, per)
    return pl.pallas_call(
        functools.partial(cross_bwd_kernel, hd ** -0.5),
        grid_spec=pltpu.PrefetchScalarGridSpec(num_scalar_prefetch=1, grid=(batch, heads // per), in_specs=[q_spec, kv_spec, p_spec, q_spec], out_specs=[q_spec, kv_spec]),
        out_shape=[jax.ShapeDtypeStruct(q.shape, BF), jax.ShapeDtypeStruct(kv.shape, BF)],
        cost_estimate=pl.CostEstimate(flops=8 * batch * heads * hd * blk * slots * 8, bytes_accessed=batch * heads * blk * (hd * 6 + slots * 2), transcendentals=0),
        compiler_params=pltpu.CompilerParams(vmem_limit_bytes=32 << 20),
        name="cross_bwd",
    )(lens, q, kv, prob, g)


def entry_barrier(me):
    barrier = pltpu.get_barrier_semaphore()
    for k in range(1, N_DEV):
        pl.semaphore_signal(barrier, inc=1, device_id={"tp": me ^ k}, device_id_type=pl.DeviceIdType.MESH)
    pl.semaphore_wait(barrier, N_DEV - 1)


def block_copy(src, dst, send_sem, recv_sem, peer, k):
    if k == 0:
        return pltpu.make_async_copy(src, dst, recv_sem)
    return pltpu.make_async_remote_copy(src_ref=src, dst_ref=dst, send_sem=send_sem, recv_sem=recv_sem, device_id={"tp": peer}, device_id_type=pl.DeviceIdType.MESH)


def to_tokens_kernel(rows, *refs):
    count = len(refs) - 3
    srcs, dst, send, recv = refs[:count], refs[count], refs[count + 1], refs[count + 2]
    me = lax.axis_index("tp")
    blk = dst.shape[-1]
    entry_barrier(me)
    copies = []
    for b, src in enumerate(srcs):
        for k in range(N_DEV):
            peer = me ^ k
            part = src.at[:, :, pl.ds(pl.multiple_of(peer * blk, blk), blk)]
            copies.append(block_copy(part, dst.at[b, pl.ds(me * rows, rows)], send.at[b, k], recv.at[b, k], peer, k))
    for copy in copies:
        copy.start()
    for copy in copies:
        copy.wait()


def to_tokens(*srcs):
    rows, hd, tokens = srcs[0].shape
    count = len(srcs)
    return pl.pallas_call(
        functools.partial(to_tokens_kernel, rows),
        in_specs=[pl.BlockSpec(memory_space=pltpu.VMEM)] * count,
        out_specs=pl.BlockSpec(memory_space=pltpu.VMEM),
        out_shape=jax.ShapeDtypeStruct((count, N_DEV * rows, hd, tokens // N_DEV), BF),
        scratch_shapes=[pltpu.SemaphoreType.DMA((count, N_DEV)), pltpu.SemaphoreType.DMA((count, N_DEV))],
        compiler_params=pltpu.CompilerParams(collective_id=rows, has_side_effects=True, vmem_limit_bytes=32 << 20),
        name="to_tokens",
    )(*srcs)


def to_heads_kernel(rows, src, dst, send, recv):
    me = lax.axis_index("tp")
    blk = src.shape[-1]
    entry_barrier(me)
    copies = []
    for b in range(src.shape[0]):
        for k in range(N_DEV):
            peer = me ^ k
            part = dst.at[b, :, :, pl.ds(pl.multiple_of(me * blk, blk), blk)]
            copies.append(block_copy(src.at[b, pl.ds(peer * rows, rows)], part, send.at[b, k], recv.at[b, k], peer, k))
    for copy in copies:
        copy.start()
    for copy in copies:
        copy.wait()


def to_heads(src):
    batch, heads, hd, blk = src.shape
    rows = heads // N_DEV
    return pl.pallas_call(
        functools.partial(to_heads_kernel, rows),
        in_specs=[pl.BlockSpec(memory_space=pltpu.VMEM)],
        out_specs=pl.BlockSpec(memory_space=pltpu.VMEM),
        out_shape=jax.ShapeDtypeStruct((batch, rows, hd, N_DEV * blk), BF),
        scratch_shapes=[pltpu.SemaphoreType.DMA((batch, N_DEV)), pltpu.SemaphoreType.DMA((batch, N_DEV))],
        compiler_params=pltpu.CompilerParams(collective_id=9, has_side_effects=True, vmem_limit_bytes=32 << 20),
        name="to_heads",
    )(src)


def gather_rows(tensor):
    return lax.all_gather(tensor, 'tp', axis=0, tiled=True)


def scatter_rows(tensor):
    return lax.psum_scatter(tensor.astype(BF), 'tp', scatter_dimension=0, tiled=True)


def device_block(x_loc, y_loc, t_loc, len_loc, mod_table, w_qkv, b_qkv, w_o, b_o, w_q, b_q, w_kv, b_kv, w_co, b_co, w_1, b_1, w_2, b_2, g_loc):
    batch, n_loc, width = x_loc.shape
    heads_loc, head_dim = w_q.shape[1], w_q.shape[2]
    heads = heads_loc * N_DEV
    inner = heads * head_dim
    slots_loc = y_loc.shape[1]
    slots = slots_loc * N_DEV
    slots_pad = 128
    ffn_loc = w_1.shape[1]
    ffn = ffn_loc * N_DEV
    mod_rows = mod_table.astype(F32)[None] + t_loc.astype(F32).reshape(batch, 6, width)
    shift1, scale1, gate1, shift2, scale2, gate2 = [mod_rows[:, row_idx, None, :] for row_idx in range(6)]

    normed1, inv_std1 = layer_norm(x_loc)
    h1 = (normed1 * (1.0 + scale1) + shift1).astype(BF)
    h1_all = [gather_rows(h1[b]) for b in range(batch)]

    wqkv_t = w_qkv.transpose(1, 2, 0)
    wkv_t = w_kv.transpose(1, 2, 0)
    wq_t = w_q.transpose(1, 2, 0).reshape(heads_loc * head_dim, width)
    w1_t = w_1.T
    small = jnp.concatenate([b_q.reshape(-1), b_1])
    small = jnp.pad(small, (0, width - small.shape[0]))[None]
    misc = jnp.concatenate([y_loc.reshape(batch * slots_loc, width), small], axis=0)
    misc = jnp.pad(misc, ((0, 64 - misc.shape[0]), (0, 0)))
    misc_all = gather_rows(misc).reshape(N_DEV, 64, width)
    y_all = misc_all[:, :batch * slots_loc].reshape(N_DEV, batch, slots_loc, width).transpose(1, 0, 2, 3).reshape(batch, slots, width)
    y_all = jnp.pad(y_all, ((0, 0), (0, slots_pad - slots), (0, 0)))
    small_all = misc_all[:, batch * slots_loc]
    bq_all = small_all[:, :heads_loc * head_dim].reshape(inner)
    b1_all = small_all[:, heads_loc * head_dim:heads_loc * head_dim + ffn_loc].reshape(ffn)
    wo_all = gather_rows(w_o.reshape(heads_loc * head_dim, width))
    wq_all = gather_rows(wq_t)
    wco_all = gather_rows(w_co.reshape(heads_loc * head_dim, width))
    w1_all = gather_rows(w1_t)
    w2_all = gather_rows(w_2)
    wqkv_all = gather_rows(wqkv_t.reshape(heads_loc * 3 * head_dim, width))

    qkv, o_heads, lse = [], [], []
    for b in range(batch):
        qkv_b = (product('hed,td->het', wqkv_t, h1_all[b]) + b_qkv[:, :, None]).astype(BF)
        qkv.append(qkv_b.reshape(heads_loc, 3, head_dim, N_DEV * n_loc))
        o_b, lse_b = attn_fwd(qkv[b])
        o_heads.append(o_b)
        lse.append(lse_b)
    o_tok = to_tokens(*o_heads).reshape(batch, inner, n_loc)

    kv_t = (product('hed,bsd->bhes', wkv_t, y_all) + b_kv[None, :, :, None]).astype(BF)
    kv_all = gather_rows(kv_t.reshape(1, batch, heads_loc, 2, head_dim, slots_pad))

    attn_total = product('bet,ed->btd', o_tok, wo_all) + b_o
    x1 = (x_loc + gate1 * attn_total).astype(BF)
    q_cross = (product('ed,btd->bet', wq_all, x1) + bq_all[None, :, None]).astype(BF)
    q_cross = q_cross.reshape(batch, heads, head_dim, n_loc)
    cross_val, cross_prob = cross_fwd(len_loc, q_cross, kv_all)
    cross_rows = cross_val.reshape(batch, inner, n_loc)
    x2 = (x1 + (product('bet,ed->btd', cross_rows, wco_all) + b_co)).astype(BF)

    normed2, inv_std2 = layer_norm(x2)
    h2 = (normed2 * (1.0 + scale2) + shift2).astype(BF)
    hidden = product('btd,fd->btf', h2, w1_all) + b1_all
    gelu_out, gelu_vjp = jax.vjp(gelu_tanh, hidden)
    gelu_out = gelu_out.astype(BF)
    mlp_total = product('btf,fd->btd', gelu_out, w2_all) + b_2
    x_out = (x2 + gate2 * mlp_total).astype(BF)

    g_x2 = g_loc.astype(F32)
    g_gate2 = jnp.sum(g_x2 * mlp_total, axis=(0, 1))
    g_mlp_f = g_x2 * gate2
    g_b_2 = jnp.sum(g_mlp_f, axis=(0, 1))
    g_mlp = g_mlp_f.astype(BF)
    g_w_2 = scatter_rows(product('btf,btd->fd', gelu_out, g_mlp))
    g_hidden = gelu_vjp(product('btd,fd->btf', g_mlp, w2_all))[0]
    g_b_1 = jnp.sum(g_hidden, axis=(0, 1))
    g_hidden = g_hidden.astype(BF)
    g_w_1 = scatter_rows(product('btf,btd->fd', g_hidden, h2)).T
    g_h2 = product('btf,fd->btd', g_hidden, w1_all)
    g_shift2 = jnp.sum(g_h2, axis=(0, 1))
    g_scale2 = jnp.sum(g_h2 * normed2, axis=(0, 1))
    g_x2 = g_x2 + layer_norm_back(normed2, inv_std2, g_h2 * (1.0 + scale2))

    g_b_co = jnp.sum(g_x2, axis=(0, 1))
    g_cross = g_x2.astype(BF)
    g_w_co = scatter_rows(product('bet,btd->ed', cross_rows, g_cross))
    g_cross_val = product('btd,ed->bet', g_cross, wco_all).astype(BF).reshape(batch, heads, head_dim, n_loc)
    g_q, g_kv = cross_bwd(len_loc, q_cross, kv_all, cross_prob, g_cross_val)
    g_q = g_q.reshape(batch, inner, n_loc)
    g_b_q = jnp.sum(g_q.astype(F32), axis=(0, 2))
    g_w_q = scatter_rows(product('bet,btd->ed', g_q, x1))
    g_x1 = g_x2 + product('bet,ed->btd', g_q, wq_all)
    g_kv = scatter_rows(g_kv).reshape(batch, heads_loc, 2 * head_dim, slots_pad)
    g_b_kv = jnp.sum(g_kv.astype(F32), axis=(0, 3))
    g_w_kv = product('bhes,bsd->hed', g_kv, y_all).astype(BF).transpose(2, 0, 1)
    g_y = lax.psum_scatter(product('bhes,hed->bsd', g_kv, wkv_t)[:, :slots].astype(BF), 'tp', scatter_dimension=1, tiled=True)

    g_gate1 = jnp.sum(g_x1 * attn_total, axis=(0, 1))
    g_attn_f = g_x1 * gate1
    g_b_o = jnp.sum(g_attn_f, axis=(0, 1))
    g_attn = g_attn_f.astype(BF)
    g_w_o = scatter_rows(product('bet,btd->ed', o_tok, g_attn))
    g_o = product('btd,ed->bet', g_attn, wo_all).astype(BF).reshape(batch, heads, head_dim, n_loc)
    g_o = to_heads(g_o)
    g_qkv = [attn_bwd(qkv[b], o_heads[b], lse[b], g_o[b]) for b in range(batch)]
    g_qkv_tok = to_tokens(*[g.reshape(heads_loc * 3, head_dim, N_DEV * n_loc) for g in g_qkv])
    g_h1 = product('bet,ed->btd', g_qkv_tok.reshape(batch, 3 * inner, n_loc), wqkv_all)
    g_rows = [g.reshape(heads_loc, 3 * head_dim, N_DEV * n_loc) for g in g_qkv]
    g_b_qkv = sum(jnp.sum(g.astype(F32), axis=2) for g in g_rows)
    g_w_qkv = sum(product('het,td->hed', g_rows[b], h1_all[b]) for b in range(batch)).astype(BF).transpose(2, 0, 1)
    g_x = g_x1 + layer_norm_back(normed1, inv_std1, g_h1 * (1.0 + scale1))
    rows = [jnp.sum(g_h1, axis=(0, 1)), jnp.sum(g_h1 * normed1, axis=(0, 1)), g_gate1, g_shift2, g_scale2, g_gate2, g_b_o, g_b_q, g_b_co, g_b_2]
    total = lax.psum(jnp.concatenate([jnp.stack(rows), g_b_1.reshape(ffn // width, width)], axis=0), 'tp')
    me = lax.axis_index('tp')
    g_b_q = lax.dynamic_slice(total[7], (me * heads_loc * head_dim,), (heads_loc * head_dim,)).reshape(heads_loc, head_dim)
    g_b_1 = lax.dynamic_slice(total[10:].reshape(ffn), (me * ffn_loc,), (ffn_loc,))

    return (x_out, g_x.astype(BF), g_y, total[:6], g_w_qkv, g_b_qkv.astype(BF), g_w_o.reshape(heads_loc, head_dim, width), total[6].astype(BF), g_w_q.reshape(heads_loc, head_dim, width).transpose(2, 0, 1), g_b_q.astype(BF), g_w_kv, g_b_kv.astype(BF), g_w_co.reshape(heads_loc, head_dim, width), total[8].astype(BF), g_w_1, g_b_1.astype(BF), g_w_2, total[9].astype(BF))


def solution(mesh):
    token_spec = P('dp', 'tp', None)
    group_rows = ('dp', 'tp')
    in_specs = (token_spec, token_spec, P('dp', None), P('dp'), P(None, None), P(None, 'tp', None), P('tp', None), P('tp', None, None), P(None), P(None, 'tp', None), P('tp', None), P(None, 'tp', None), P('tp', None), P('tp', None, None), P(None), P(None, 'tp'), P('tp'), P('tp', None), P(None), token_spec)
    out_specs = (token_spec, token_spec, token_spec, P('dp', None), P('dp', 'tp', None), P(group_rows, None), P(group_rows, None, None), P('dp'), P('dp', 'tp', None), P(group_rows, None), P('dp', 'tp', None), P(group_rows, None), P(group_rows, None, None), P('dp'), P('dp', 'tp'), P(group_rows), P(group_rows, None), P('dp'))
    return jax.shard_map(device_block, mesh=mesh, in_specs=in_specs, out_specs=out_specs, check_vma=False)
```

```python
import functools
import math

import jax
import jax.numpy as jnp
from jax import lax
from jax.experimental import pallas as pl
from jax.experimental.pallas import tpu as pltpu
from jax.sharding import PartitionSpec as P

LN_EPS = 1e-6
MASK_FILL = -1e30
N_DEV = 8
TP = ('y', 'x', 'c')
ROW = ('x', 'c')
LOG2E = math.log2(math.e)
BF = jnp.bfloat16
F32 = jnp.float32


def product(form, lhs, rhs):
    return jnp.einsum(form, lhs, rhs, preferred_element_type=F32)


def layer_norm(tensor):
    tensor = tensor.astype(F32)
    centered = tensor - jnp.mean(tensor, axis=-1, keepdims=True)
    inv_std = lax.rsqrt(jnp.mean(centered * centered, axis=-1, keepdims=True) + LN_EPS)
    return centered * inv_std, inv_std


def layer_norm_back(normed, inv_std, g_normed):
    mean_g = jnp.mean(g_normed, axis=-1, keepdims=True)
    mean_gn = jnp.mean(g_normed * normed, axis=-1, keepdims=True)
    return inv_std * (g_normed - mean_g - normed * mean_gn)


def gelu_tanh(tensor):
    return jax.nn.gelu(tensor, approximate=True)


def dot00(lhs, rhs):
    return lax.dot_general(lhs, rhs, (((0,), (0,)), ((), ())), preferred_element_type=F32)


def dot10(lhs, rhs):
    return lax.dot_general(lhs, rhs, (((1,), (0,)), ((), ())), preferred_element_type=F32)


def dot11(lhs, rhs):
    return lax.dot_general(lhs, rhs, (((1,), (1,)), ((), ())), preferred_element_type=F32)


def attn_fwd_kernel(scale, blk, qkv_ref, o_ref, lse_ref):
    tokens = o_ref.shape[2]
    factor = scale * LOG2E

    def step(j, carry):
        cols = pl.ds(pl.multiple_of(j * blk, blk), blk)
        s = dot00(qkv_ref[0, 1], qkv_ref[0, 0, :, cols])
        top = jnp.max(s, axis=0, keepdims=True) * factor
        p = jnp.exp2(s * factor - top)
        total = jnp.sum(p, axis=0, keepdims=True)
        o = dot10(qkv_ref[0, 2], p.astype(BF))
        o_ref[0, :, cols] = (o / total).astype(BF)
        lse_ref[0, :, cols] = top + jnp.log2(total)
        return carry

    lax.fori_loop(0, tokens // blk, step, 0)


def attn_fwd(qkv, blk=256):
    heads, _, hd, tokens = qkv.shape
    return pl.pallas_call(
        functools.partial(attn_fwd_kernel, hd ** -0.5, blk),
        grid=(heads,),
        in_specs=[pl.BlockSpec((1, 3, hd, tokens), lambda h: (h, 0, 0, 0))],
        out_specs=[pl.BlockSpec((1, hd, tokens), lambda h: (h, 0, 0)), pl.BlockSpec((1, 1, tokens), lambda h: (h, 0, 0))],
        out_shape=[jax.ShapeDtypeStruct((heads, hd, tokens), BF), jax.ShapeDtypeStruct((heads, 1, tokens), F32)],
        cost_estimate=pl.CostEstimate(flops=4 * heads * hd * tokens * tokens, bytes_accessed=heads * hd * tokens * 8, transcendentals=heads * tokens * tokens),
        compiler_params=pltpu.CompilerParams(vmem_limit_bytes=48 << 20),
        name="attn_fwd",
    )(qkv)


def attn_bwd_kernel(scale, blk, qkv_ref, o_ref, lse_ref, g_ref, d_ref, dk_acc, dv_acc):
    tokens = o_ref.shape[2]
    factor = scale * LOG2E
    dk_acc[...] = jnp.zeros_like(dk_acc)
    dv_acc[...] = jnp.zeros_like(dv_acc)

    def step(j, carry):
        cols = pl.ds(pl.multiple_of(j * blk, blk), blk)
        q = qkv_ref[0, 0, :, cols]
        g = g_ref[0, :, cols]
        delta = jnp.sum(g.astype(F32) * o_ref[0, :, cols].astype(F32), axis=0, keepdims=True)
        s = dot00(qkv_ref[0, 1], q)
        p = jnp.exp2(s * factor - lse_ref[0, :, cols])
        dp = dot00(qkv_ref[0, 2], g)
        ds = (p * (dp - delta)).astype(BF)
        dv_acc[...] += dot11(g, p.astype(BF))
        dk_acc[...] += dot11(q, ds)
        d_ref[0, 0, :, cols] = (dot10(qkv_ref[0, 1], ds) * scale).astype(BF)
        return carry

    lax.fori_loop(0, tokens // blk, step, 0)
    d_ref[0, 1] = (dk_acc[...] * scale).astype(BF)
    d_ref[0, 2] = dv_acc[...].astype(BF)


def attn_bwd(qkv, o, lse, g, blk=256):
    heads, _, hd, tokens = qkv.shape
    row = lambda h: (h, 0, 0)
    return pl.pallas_call(
        functools.partial(attn_bwd_kernel, hd ** -0.5, blk),
        grid=(heads,),
        in_specs=[pl.BlockSpec((1, 3, hd, tokens), lambda h: (h, 0, 0, 0)), pl.BlockSpec((1, hd, tokens), row), pl.BlockSpec((1, 1, tokens), row), pl.BlockSpec((1, hd, tokens), row)],
        out_specs=pl.BlockSpec((1, 3, hd, tokens), lambda h: (h, 0, 0, 0)),
        out_shape=jax.ShapeDtypeStruct((heads, 3, hd, tokens), BF),
        scratch_shapes=[pltpu.VMEM((hd, tokens), F32), pltpu.VMEM((hd, tokens), F32)],
        cost_estimate=pl.CostEstimate(flops=10 * heads * hd * tokens * tokens, bytes_accessed=heads * hd * tokens * 20, transcendentals=heads * tokens * tokens),
        compiler_params=pltpu.CompilerParams(vmem_limit_bytes=48 << 20),
        name="attn_bwd",
    )(qkv, o, lse, g)


def cross_fwd_kernel(scale, len_ref, q_ref, kv_ref, c_ref, p_ref):
    heads, slots = q_ref.shape[1], kv_ref.shape[5]
    blk = q_ref.shape[3]
    count = len_ref[pl.program_id(0)]
    ok = lax.broadcasted_iota(jnp.int32, (slots, blk), 0) < count
    for h in range(heads):
        s = dot00(kv_ref[h // 2, 0, h % 2, 0], q_ref[0, h]) * scale
        s = jnp.where(ok, s, MASK_FILL)
        p = jnp.exp(s - jnp.max(s, axis=0, keepdims=True))
        p = (p / jnp.sum(p, axis=0, keepdims=True)).astype(BF)
        p_ref[0, h] = p
        c_ref[0, h] = dot10(kv_ref[h // 2, 0, h % 2, 1], p).astype(BF)


def cross_specs(hd, blk, slots, per):
    q_spec = pl.BlockSpec((1, per, hd, blk), lambda b, i, n: (b, i, 0, 0))
    kv_spec = pl.BlockSpec((per // 2, 1, 2, 2, hd, slots), lambda b, i, n: (i, b, 0, 0, 0, 0))
    p_spec = pl.BlockSpec((1, per, slots, blk), lambda b, i, n: (b, i, 0, 0))
    return q_spec, kv_spec, p_spec


def cross_fwd(lens, q, kv, per=8):
    batch, heads, hd, blk = q.shape
    slots = kv.shape[5]
    q_spec, kv_spec, p_spec = cross_specs(hd, blk, slots, per)
    return pl.pallas_call(
        functools.partial(cross_fwd_kernel, hd ** -0.5),
        grid_spec=pltpu.PrefetchScalarGridSpec(num_scalar_prefetch=1, grid=(batch, heads // per), in_specs=[q_spec, kv_spec], out_specs=[q_spec, p_spec]),
        out_shape=[jax.ShapeDtypeStruct(q.shape, BF), jax.ShapeDtypeStruct((batch, heads, slots, blk), BF)],
        cost_estimate=pl.CostEstimate(flops=4 * batch * heads * hd * blk * slots * 8, bytes_accessed=batch * heads * blk * (hd * 4 + slots * 2), transcendentals=batch * heads * blk * slots),
        compiler_params=pltpu.CompilerParams(vmem_limit_bytes=32 << 20),
        name="cross_fwd",
    )(lens, q, kv)


def cross_bwd_kernel(scale, len_ref, q_ref, kv_ref, p_ref, g_ref, gq_ref, gkv_ref):
    heads = q_ref.shape[1]
    for h in range(heads):
        k, v = kv_ref[h // 2, 0, h % 2, 0], kv_ref[h // 2, 0, h % 2, 1]
        q, g, p = q_ref[0, h], g_ref[0, h], p_ref[0, h]
        dp = dot00(v, g)
        pf = p.astype(F32)
        delta = jnp.sum(dp * pf, axis=0, keepdims=True)
        ds = (pf * (dp - delta) * scale).astype(BF)
        gq_ref[0, h] = dot10(k, ds).astype(BF)
        gkv_ref[h // 2, 0, h % 2, 0] = dot11(q, ds).astype(BF)
        gkv_ref[h // 2, 0, h % 2, 1] = dot11(g, p).astype(BF)


def cross_bwd(lens, q, kv, prob, g, per=8):
    batch, heads, hd, blk = q.shape
    slots = kv.shape[5]
    q_spec, kv_spec, p_spec = cross_specs(hd, blk, slots, per)
    return pl.pallas_call(
        functools.partial(cross_bwd_kernel, hd ** -0.5),
        grid_spec=pltpu.PrefetchScalarGridSpec(num_scalar_prefetch=1, grid=(batch, heads // per), in_specs=[q_spec, kv_spec, p_spec, q_spec], out_specs=[q_spec, kv_spec]),
        out_shape=[jax.ShapeDtypeStruct(q.shape, BF), jax.ShapeDtypeStruct(kv.shape, BF)],
        cost_estimate=pl.CostEstimate(flops=8 * batch * heads * hd * blk * slots * 8, bytes_accessed=batch * heads * blk * (hd * 6 + slots * 2), transcendentals=0),
        compiler_params=pltpu.CompilerParams(vmem_limit_bytes=32 << 20),
        name="cross_bwd",
    )(lens, q, kv, prob, g)


def my_index():
    return lax.axis_index('y') * 4 + lax.axis_index('x') * 2 + lax.axis_index('c')


def device(index):
    return {'y': index // 4, 'x': (index // 2) % 2, 'c': index % 2}


def entry_barrier(me):
    barrier = pltpu.get_barrier_semaphore()
    for k in range(1, N_DEV):
        pl.semaphore_signal(barrier, inc=1, device_id=device(me ^ k), device_id_type=pl.DeviceIdType.MESH)
    pl.semaphore_wait(barrier, N_DEV - 1)


def block_copy(src, dst, send_sem, recv_sem, peer, k):
    if k == 0:
        return pltpu.make_async_copy(src, dst, recv_sem)
    return pltpu.make_async_remote_copy(src_ref=src, dst_ref=dst, send_sem=send_sem, recv_sem=recv_sem, device_id=device(peer), device_id_type=pl.DeviceIdType.MESH)


def exchange_kernel(moves, n_in, n_out, *refs):
    srcs, dsts, (send, recv) = refs[:n_in], refs[n_in:n_in + n_out], refs[n_in + n_out:]
    me = my_index()
    entry_barrier(me)
    copies = []
    for m, (i, take, o, put) in enumerate(moves):
        for k in range(N_DEV):
            peer = me ^ k
            copies.append(block_copy(take(srcs[i], peer), put(dsts[o], me), send.at[m, k], recv.at[m, k], peer, k))
    for copy in copies:
        copy.start()
    for copy in copies:
        copy.wait()


def exchange(name, collective_id, srcs, outs, moves):
    space = pl.BlockSpec(memory_space=pltpu.VMEM)
    return pl.pallas_call(
        functools.partial(exchange_kernel, moves, len(srcs), len(outs)),
        in_specs=[space] * len(srcs), out_specs=[space] * len(outs), out_shape=outs,
        scratch_shapes=[pltpu.SemaphoreType.DMA((len(moves), N_DEV)), pltpu.SemaphoreType.DMA((len(moves), N_DEV))],
        compiler_params=pltpu.CompilerParams(collective_id=collective_id, has_side_effects=True, vmem_limit_bytes=40 << 20),
        name=name,
    )(*srcs)


def block_at(index, blk):
    return pl.ds(pl.multiple_of(index * blk, blk), blk)


def tokens_moves(count, rows, blk):
    return [(b, lambda src, peer: src.at[:, :, block_at(peer, blk)], 0, lambda dst, me, b=b: dst.at[b, pl.ds(me * rows, rows)]) for b in range(count)]


def heads_moves(count, rows, blk):
    return [(0, lambda src, peer, b=b: src.at[b, pl.ds(peer * rows, rows)], 0, lambda dst, me, b=b: dst.at[b, :, :, block_at(me, blk)]) for b in range(count)]


def part_move(index):
    return (index, lambda src, peer: src.at[peer], index, lambda dst, me: dst.at[me])


def whole_move(index):
    return (index, lambda src, peer: src, index, lambda dst, me: dst.at[me])


def gather_rows(tensor, axes=TP):
    return lax.all_gather(tensor, axes, axis=0, tiled=True)


def scatter_rows(tensor, axes=TP):
    return lax.psum_scatter(tensor.astype(BF), axes, scatter_dimension=0, tiled=True)


def swap_y(tensor):
    return lax.ppermute(tensor, 'y', [(0, 1), (1, 0)])


def mlp_half(h2, g_mlp, w1_half, b1_half, w2_half):
    hidden = product('btd,fd->btf', h2, w1_half) + b1_half
    gelu_out, gelu_vjp = jax.vjp(gelu_tanh, hidden)
    gelu_out = gelu_out.astype(BF)
    g_hidden = gelu_vjp(product('btd,fd->btf', g_mlp, w2_half))[0]
    g_b_1 = jnp.sum(g_hidden, axis=(0, 1))
    g_hidden = g_hidden.astype(BF)
    g_h2 = product('btf,fd->btd', g_hidden, w1_half)
    part = product('btf,fd->btd', gelu_out, w2_half)
    return gelu_out, part, g_hidden, g_b_1, g_h2


def device_block(x_loc, y_loc, t_loc, len_loc, mod_table, w_qkv, b_qkv, w_o, b_o, w_q, b_q, w_kv, b_kv, w_co, b_co, w_1, b_1, w_2, b_2, g_loc):
    batch, n_loc, width = x_loc.shape
    heads_loc, head_dim = w_q.shape[1], w_q.shape[2]
    heads = heads_loc * N_DEV
    inner = heads * head_dim
    slots_loc = y_loc.shape[1]
    slots = slots_loc * N_DEV
    slots_pad = 128
    ffn_loc = w_1.shape[1]
    ffn = ffn_loc * N_DEV
    mod_rows = mod_table.astype(F32)[None] + t_loc.astype(F32).reshape(batch, 6, width)
    shift1, scale1, gate1, shift2, scale2, gate2 = [mod_rows[:, row_idx, None, :] for row_idx in range(6)]

    g_x2 = g_loc.astype(F32)
    g_mlp_f = g_x2 * gate2
    g_b_2 = jnp.sum(g_mlp_f, axis=(0, 1))
    g_mlp = g_mlp_f.astype(BF)
    g_mlp_far = swap_y(g_mlp)

    normed1, inv_std1 = layer_norm(x_loc)
    h1 = (normed1 * (1.0 + scale1) + shift1).astype(BF)
    h1_all = [gather_rows(h1[b]) for b in range(batch)]

    wqkv_t = w_qkv.transpose(1, 2, 0)
    wkv_t = w_kv.transpose(1, 2, 0)
    wq_t = w_q.transpose(1, 2, 0).reshape(heads_loc * head_dim, width)
    w1_t = w_1.T
    small = jnp.concatenate([b_q.reshape(-1), b_1])
    small = jnp.pad(small, (0, width - small.shape[0]))[None]
    misc = jnp.concatenate([y_loc.reshape(batch * slots_loc, width), small], axis=0)
    misc = jnp.pad(misc, ((0, 64 - misc.shape[0]), (0, 0)))
    misc, h1_all[0] = lax.optimization_barrier((misc, h1_all[0]))
    misc_all = gather_rows(misc).reshape(N_DEV, 64, width)
    y_all = misc_all[:, :batch * slots_loc].reshape(N_DEV, batch, slots_loc, width).transpose(1, 0, 2, 3).reshape(batch, slots, width)
    y_all = jnp.pad(y_all, ((0, 0), (0, slots_pad - slots), (0, 0)))
    small_all = misc_all[:, batch * slots_loc]
    bq_all = small_all[:, :heads_loc * head_dim].reshape(inner)
    b1_all = small_all[:, heads_loc * head_dim:heads_loc * head_dim + ffn_loc].reshape(2, ffn // 2)
    b1_half = lax.dynamic_index_in_dim(b1_all, lax.axis_index('y'), keepdims=False)
    wo_all = gather_rows(w_o.reshape(heads_loc * head_dim, width))
    wq_all = gather_rows(wq_t)
    wco_all = gather_rows(w_co.reshape(heads_loc * head_dim, width))
    w1_half = gather_rows(w1_t, ROW)
    w2_half = gather_rows(w_2, ROW)
    wqkv_all = gather_rows(wqkv_t.reshape(heads_loc * 3 * head_dim, width))

    qkv, o_heads, lse = [], [], []
    for b in range(batch):
        qkv_b = (product('hed,td->het', wqkv_t, h1_all[b]) + b_qkv[:, :, None]).astype(BF)
        qkv.append(qkv_b.reshape(heads_loc, 3, head_dim, N_DEV * n_loc))
        o_b, lse_b = attn_fwd(qkv[b])
        o_heads.append(o_b)
        lse.append(lse_b)
    shape = lambda *dims, dtype=BF: jax.ShapeDtypeStruct(dims, dtype)
    o_tok, = exchange("o_exchange", 1, o_heads, [shape(batch, heads, head_dim, n_loc)], tokens_moves(batch, heads_loc, n_loc))
    o_tok = o_tok.reshape(batch, inner, n_loc)

    kv_t = (product('hed,bsd->bhes', wkv_t, y_all) + b_kv[None, :, :, None]).astype(BF)
    kv_all = gather_rows(kv_t.reshape(1, batch, heads_loc, 2, head_dim, slots_pad))

    attn_total = product('bet,ed->btd', o_tok, wo_all) + b_o
    x1 = (x_loc + gate1 * attn_total).astype(BF)
    q_cross = (product('ed,btd->bet', wq_all, x1) + bq_all[None, :, None]).astype(BF)
    q_cross = q_cross.reshape(batch, heads, head_dim, n_loc)
    cross_val, cross_prob = cross_fwd(len_loc, q_cross, kv_all)
    cross_rows = cross_val.reshape(batch, inner, n_loc)
    x2 = (x1 + (product('bet,ed->btd', cross_rows, wco_all) + b_co)).astype(BF)

    normed2, inv_std2 = layer_norm(x2)
    h2 = (normed2 * (1.0 + scale2) + shift2).astype(BF)
    own = mlp_half(h2, g_mlp, w1_half, b1_half, w2_half)
    h2_far = swap_y(h2)
    far = mlp_half(h2_far, g_mlp_far, w1_half, b1_half, w2_half)
    g_h2_far, gelu_own, g_hid_own = lax.optimization_barrier((far[4].astype(BF), own[0], own[2]))
    g_h2 = own[4] + swap_y(g_h2_far).astype(F32)
    mlp_total = own[1] + swap_y(far[1].astype(BF)).astype(F32) + b_2
    x_out = (x2 + gate2 * mlp_total).astype(BF)
    g_gate2 = jnp.sum(g_x2 * mlp_total, axis=(0, 1))
    pair = lambda near, other: jnp.concatenate([near, other], axis=0)
    p_w_2 = product('btf,btd->fd', pair(gelu_own, far[0]), pair(g_mlp, g_mlp_far)).astype(BF)
    p_w_1 = product('btf,btd->fd', pair(g_hid_own, far[2]), pair(h2, h2_far)).astype(BF)
    g_h2, p_w_2, p_w_1, wqkv_all = lax.optimization_barrier((g_h2, p_w_2, p_w_1, wqkv_all))
    g_w_2 = scatter_rows(p_w_2, ROW)
    g_w_1 = scatter_rows(p_w_1, ROW).T
    g_b_1 = own[3] + far[3]
    g_shift2 = jnp.sum(g_h2, axis=(0, 1))
    g_scale2 = jnp.sum(g_h2 * normed2, axis=(0, 1))
    g_x2 = g_x2 + layer_norm_back(normed2, inv_std2, g_h2 * (1.0 + scale2))

    g_b_co = jnp.sum(g_x2, axis=(0, 1))
    g_cross = g_x2.astype(BF)
    p_w_co = product('bet,btd->ed', cross_rows, g_cross).astype(BF)
    g_cross_val = product('btd,ed->bet', g_cross, wco_all).astype(BF).reshape(batch, heads, head_dim, n_loc)
    g_q, g_kv = cross_bwd(len_loc, q_cross, kv_all, cross_prob, g_cross_val)
    g_q = g_q.reshape(batch, inner, n_loc)
    g_b_q = jnp.sum(g_q.astype(F32), axis=(0, 2))
    p_w_q = product('bet,btd->ed', g_q, x1).astype(BF)
    g_x1 = g_x2 + product('bet,ed->btd', g_q, wq_all)
    g_gate1 = jnp.sum(g_x1 * attn_total, axis=(0, 1))
    g_attn_f = g_x1 * gate1
    g_b_o = jnp.sum(g_attn_f, axis=(0, 1))
    g_attn = g_attn_f.astype(BF)
    p_w_o = product('bet,btd->ed', o_tok, g_attn).astype(BF)
    g_o = product('btd,ed->bet', g_attn, wo_all).astype(BF).reshape(batch, heads, head_dim, n_loc)
    g_o, p_w_co, p_w_q, p_w_o = lax.optimization_barrier((g_o, p_w_co, p_w_q, p_w_o))
    g_w_co, g_w_q, g_w_o = scatter_rows(p_w_co), scatter_rows(p_w_q), scatter_rows(p_w_o)
    g_b_1 = jnp.where(lax.axis_index('y') == jnp.arange(2)[:, None], g_b_1[None], 0.0).reshape(ffn // width, width)
    early = jnp.stack([g_gate1, g_shift2, g_scale2, g_gate2, g_b_o, g_b_q, g_b_co, g_b_2])
    early = jnp.concatenate([early, g_b_1, jnp.zeros((16 - 8 - ffn // width, width), F32)], axis=0)
    g_o, g_kv, early = exchange(
        "g_o_exchange", 2, [g_o, g_kv, early],
        [shape(batch, heads_loc, head_dim, N_DEV * n_loc), shape(*g_kv.shape), shape(N_DEV, 16, width, dtype=F32)],
        heads_moves(batch, heads_loc, n_loc) + [part_move(1), whole_move(2)])
    g_kv = jnp.sum(g_kv.astype(F32), axis=0).reshape(batch, heads_loc, 2 * head_dim, slots_pad)
    g_b_kv = jnp.sum(g_kv, axis=(0, 3))
    g_kv = g_kv.astype(BF)
    g_y = product('bhes,hed->bsd', g_kv, wkv_t)[:, :slots].astype(BF)
    g_y = g_y.reshape(batch, N_DEV, slots_loc, width).transpose(1, 0, 2, 3).reshape(N_DEV, batch * slots_loc, width)
    g_y = jnp.pad(g_y, ((0, 0), (0, 32 - batch * slots_loc), (0, 0)))
    g_qkv = [attn_bwd(qkv[b], o_heads[b], lse[b], g_o[b]) for b in range(batch)]
    g_qkv_tok, g_y = exchange(
        "g_qkv_exchange", 3, [g.reshape(heads_loc * 3, head_dim, N_DEV * n_loc) for g in g_qkv] + [g_y],
        [shape(batch, heads * 3, head_dim, n_loc), shape(*g_y.shape)],
        tokens_moves(batch, heads_loc * 3, n_loc) + [(2, part_move(0)[1], 1, part_move(0)[3])])
    g_y = jnp.sum(g_y.astype(F32), axis=0)[:batch * slots_loc].reshape(batch, slots_loc, width).astype(BF)
    g_w_kv = product('bhes,bsd->hed', g_kv, y_all).astype(BF).transpose(2, 0, 1)
    g_h1 = product('bet,ed->btd', g_qkv_tok.reshape(batch, 3 * inner, n_loc), wqkv_all)
    g_rows = [g.reshape(heads_loc, 3 * head_dim, N_DEV * n_loc) for g in g_qkv]
    g_b_qkv = sum(jnp.sum(g.astype(F32), axis=2) for g in g_rows)
    g_w_qkv = sum(product('het,td->hed', g_rows[b], h1_all[b]) for b in range(batch)).astype(BF).transpose(2, 0, 1)
    g_x = g_x1 + layer_norm_back(normed1, inv_std1, g_h1 * (1.0 + scale1))
    late = jnp.stack([jnp.sum(g_h1, axis=(0, 1)), jnp.sum(g_h1 * normed1, axis=(0, 1))])
    late = jnp.pad(late, ((0, 6), (0, 0)))
    late, g_w_2, g_w_1 = lax.optimization_barrier((late, g_w_2, g_w_1))
    late, = exchange("late_exchange", 4, [late], [shape(N_DEV, 8, width, dtype=F32)], [whole_move(0)])
    late = jnp.sum(late, axis=0)
    early = jnp.sum(early, axis=0)
    me = my_index()
    g_b_q = lax.dynamic_slice(early[5], (me * heads_loc * head_dim,), (heads_loc * head_dim,)).reshape(heads_loc, head_dim)
    g_b_1 = lax.dynamic_slice(early[8:8 + ffn // width].reshape(ffn), (me * ffn_loc,), (ffn_loc,))

    return (x_out, g_x.astype(BF), g_y, jnp.concatenate([late[:2], early[:4]], axis=0), g_w_qkv, g_b_qkv.astype(BF), g_w_o.reshape(heads_loc, head_dim, width), early[4].astype(BF), g_w_q.reshape(heads_loc, head_dim, width).transpose(2, 0, 1), g_b_q.astype(BF), g_w_kv, g_b_kv.astype(BF), g_w_co.reshape(heads_loc, head_dim, width), early[6].astype(BF), g_w_1, g_b_1.astype(BF), g_w_2, early[7].astype(BF))


def solution(mesh):
    mesh = jax.sharding.Mesh(mesh.devices.reshape(-1, 2, 2, 2), ('dp',) + TP)
    token_spec = P('dp', TP, None)
    group_rows = ('dp',) + TP
    in_specs = (token_spec, token_spec, P('dp', None), P('dp'), P(None, None), P(None, TP, None), P(TP, None), P(TP, None, None), P(None), P(None, TP, None), P(TP, None), P(None, TP, None), P(TP, None), P(TP, None, None), P(None), P(None, TP), P(TP), P(TP, None), P(None), token_spec)
    out_specs = (token_spec, token_spec, token_spec, P('dp', None), P('dp', TP, None), P(group_rows, None), P(group_rows, None, None), P('dp'), P('dp', TP, None), P(group_rows, None), P('dp', TP, None), P(group_rows, None), P(group_rows, None, None), P('dp'), P('dp', TP), P(group_rows), P(group_rows, None), P('dp'))
    return jax.shard_map(device_block, mesh=mesh, in_specs=in_specs, out_specs=out_specs, check_vma=False)
```

```python
import functools
import math

import jax
import jax.numpy as jnp
from jax import lax
from jax.experimental import pallas as pl
from jax.experimental.pallas import tpu as pltpu
from jax.sharding import PartitionSpec as P

LN_EPS = 1e-6
MASK_FILL = -1e30
N_DEV = 8
TP = ('y', 'x', 'c')
ROW = ('x', 'c')
LOG2E = math.log2(math.e)
BF = jnp.bfloat16
F32 = jnp.float32


def product(form, lhs, rhs):
    return jnp.einsum(form, lhs, rhs, preferred_element_type=F32)


def layer_norm(tensor):
    tensor = tensor.astype(F32)
    centered = tensor - jnp.mean(tensor, axis=-1, keepdims=True)
    inv_std = lax.rsqrt(jnp.mean(centered * centered, axis=-1, keepdims=True) + LN_EPS)
    return centered * inv_std, inv_std


def layer_norm_back(normed, inv_std, g_normed):
    mean_g = jnp.mean(g_normed, axis=-1, keepdims=True)
    mean_gn = jnp.mean(g_normed * normed, axis=-1, keepdims=True)
    return inv_std * (g_normed - mean_g - normed * mean_gn)


def gelu_tanh(tensor):
    return jax.nn.gelu(tensor, approximate=True)


def dot00(lhs, rhs):
    return lax.dot_general(lhs, rhs, (((0,), (0,)), ((), ())), preferred_element_type=F32)


def dot10(lhs, rhs):
    return lax.dot_general(lhs, rhs, (((1,), (0,)), ((), ())), preferred_element_type=F32)


def dot11(lhs, rhs):
    return lax.dot_general(lhs, rhs, (((1,), (1,)), ((), ())), preferred_element_type=F32)


def my_index():
    return lax.axis_index('y') * 4 + lax.axis_index('x') * 2 + lax.axis_index('c')


def device(index):
    return {'y': index // 4, 'x': (index // 2) % 2, 'c': index % 2}


def entry_barrier(me):
    barrier = pltpu.get_barrier_semaphore()
    for k in range(1, N_DEV):
        pl.semaphore_signal(barrier, inc=1, device_id=device(me ^ k), device_id_type=pl.DeviceIdType.MESH)
    pl.semaphore_wait(barrier, N_DEV - 1)


def block_copy(src, dst, send_sem, recv_sem, peer, k):
    if k == 0:
        return pltpu.make_async_copy(src, dst, recv_sem)
    return pltpu.make_async_remote_copy(src_ref=src, dst_ref=dst, send_sem=send_sem, recv_sem=recv_sem, device_id=device(peer), device_id_type=pl.DeviceIdType.MESH)


def start_all(copies):
    for copy in copies:
        copy.start()


def wait_all(copies):
    for copy in copies:
        copy.wait()


def block_at(index, blk):
    return pl.ds(pl.multiple_of(index * blk, blk), blk)


def late_kernel(parts, whole, parts_out, whole_out, send, recv):
    me = my_index()
    entry_barrier(me)
    copies = []
    for k in range(N_DEV):
        peer = me ^ k
        copies.append(block_copy(parts.at[peer], parts_out.at[me], send.at[0, k], recv.at[0, k], peer, k))
        copies.append(block_copy(whole, whole_out.at[me], send.at[1, k], recv.at[1, k], peer, k))
    start_all(copies)
    wait_all(copies)


def late_exchange(parts, whole):
    space = pl.BlockSpec(memory_space=pltpu.VMEM)
    return pl.pallas_call(
        late_kernel, in_specs=[space] * 2, out_specs=[space] * 2,
        out_shape=[jax.ShapeDtypeStruct(parts.shape, parts.dtype), jax.ShapeDtypeStruct((N_DEV,) + whole.shape, whole.dtype)],
        scratch_shapes=[pltpu.SemaphoreType.DMA((2, N_DEV)), pltpu.SemaphoreType.DMA((2, N_DEV))],
        compiler_params=pltpu.CompilerParams(collective_id=3, has_side_effects=True, vmem_limit_bytes=16 << 20),
        name="late_exchange",
    )(parts, whole)


def attn_fwd_kernel(scale, blk, heads, qkv_ref, kv_ref, o_ref, lse_ref, tok_ref, kv_out, o_scr, send, recv, kv_send, kv_recv):
    i = pl.program_id(0)
    last = pl.num_programs(0) - 1
    tokens = o_ref.shape[2]
    factor = scale * LOG2E
    me = my_index()

    def o_copies(step):
        return [block_copy(o_scr.at[step, :, block_at(me ^ k, blk)], tok_ref.at[step // heads, me * heads + step % heads], send.at[step, k], recv.at[step, k], me ^ k, k) for k in range(N_DEV)]

    kv_copies = [block_copy(kv_ref, kv_out.at[me], kv_send.at[k], kv_recv.at[k], me ^ k, k) for k in range(N_DEV)]

    @pl.when(i == 0)
    def _():
        entry_barrier(me)
        start_all(kv_copies)

    def step(j, carry):
        cols = block_at(j, blk)
        s = dot00(qkv_ref[0, 1], qkv_ref[0, 0, :, cols])
        top = jnp.max(s, axis=0, keepdims=True) * factor
        p = jnp.exp2(s * factor - top)
        total = jnp.sum(p, axis=0, keepdims=True)
        o = dot10(qkv_ref[0, 2], p.astype(BF))
        o_scr[i, :, cols] = (o / total).astype(BF)
        lse_ref[0, :, cols] = top + jnp.log2(total)
        return carry

    lax.fori_loop(0, tokens // blk, step, 0)
    o_ref[0] = o_scr[i]
    start_all(o_copies(i))

    @pl.when(i == last)
    def _():
        for n in range(o_scr.shape[0]):
            wait_all(o_copies(n))
        wait_all(kv_copies)


def attn_fwd(qkv, kv, heads, blk):
    steps, _, hd, tokens = qkv.shape
    batch = steps // heads
    hbm = pl.BlockSpec(memory_space=pl.ANY)
    dma = pltpu.SemaphoreType.DMA
    return pl.pallas_call(
        functools.partial(attn_fwd_kernel, hd ** -0.5, blk, heads),
        grid=(steps,),
        in_specs=[pl.BlockSpec((1, 3, hd, tokens), lambda i: (i, 0, 0, 0)), hbm],
        out_specs=[pl.BlockSpec((1, hd, tokens), lambda i: (i, 0, 0)), pl.BlockSpec((1, 1, tokens), lambda i: (i, 0, 0)), hbm, hbm],
        out_shape=[jax.ShapeDtypeStruct((steps, hd, tokens), BF), jax.ShapeDtypeStruct((steps, 1, tokens), F32),
                   jax.ShapeDtypeStruct((batch, N_DEV * heads, hd, blk), BF), jax.ShapeDtypeStruct((N_DEV,) + kv.shape, BF)],
        scratch_shapes=[pltpu.VMEM((steps, hd, tokens), BF), dma((steps, N_DEV)), dma((steps, N_DEV)), dma((N_DEV,)), dma((N_DEV,))],
        cost_estimate=pl.CostEstimate(flops=4 * steps * hd * tokens * tokens, bytes_accessed=steps * hd * tokens * 8, transcendentals=steps * tokens * tokens),
        compiler_params=pltpu.CompilerParams(collective_id=1, has_side_effects=True, vmem_limit_bytes=48 << 20),
        name="attn_fwd",
    )(qkv, kv)


def attn_bwd_kernel(scale, blk, heads, qkv_ref, o_ref, lse_ref, g_ref, kv_ref, early_ref, d_ref, tok_ref, kv_out, early_out,
                    g_scr, d_scr, dk_acc, dv_acc, g_send, g_recv, d_send, d_recv, x_send, x_recv):
    i = pl.program_id(0)
    steps = d_scr.shape[0]
    tokens = o_ref.shape[2]
    factor = scale * LOG2E
    me = my_index()

    def g_copies(step):
        return [block_copy(g_ref.at[step // heads, (me ^ k) * heads + step % heads], g_scr.at[step, :, block_at(me, blk)], g_send.at[step, k], g_recv.at[step, k], me ^ k, k) for k in range(N_DEV)]

    def d_copies(step):
        return [block_copy(d_scr.at[step, :, :, block_at(me ^ k, blk)], tok_ref.at[step // heads, me * heads + step % heads], d_send.at[step, k], d_recv.at[step, k], me ^ k, k) for k in range(N_DEV)]

    x_copies = []
    for k in range(N_DEV):
        x_copies.append(block_copy(kv_ref.at[me ^ k], kv_out.at[me], x_send.at[0, k], x_recv.at[0, k], me ^ k, k))
        x_copies.append(block_copy(early_ref, early_out.at[me], x_send.at[1, k], x_recv.at[1, k], me ^ k, k))

    @pl.when(i == 0)
    def _():
        entry_barrier(me)
        for n in range(steps):
            start_all(g_copies(n))
        start_all(x_copies)

    wait_all(g_copies(i))
    dk_acc[...] = jnp.zeros_like(dk_acc)
    dv_acc[...] = jnp.zeros_like(dv_acc)

    def step(j, carry):
        cols = block_at(j, blk)
        q = qkv_ref[0, 0, :, cols]
        g = g_scr[i, :, cols]
        delta = jnp.sum(g.astype(F32) * o_ref[0, :, cols].astype(F32), axis=0, keepdims=True)
        s = dot00(qkv_ref[0, 1], q)
        p = jnp.exp2(s * factor - lse_ref[0, :, cols])
        dp = dot00(qkv_ref[0, 2], g)
        ds = (p * (dp - delta)).astype(BF)
        dv_acc[...] += dot11(g, p.astype(BF))
        dk_acc[...] += dot11(q, ds)
        d_scr[i, 0, :, cols] = (dot10(qkv_ref[0, 1], ds) * scale).astype(BF)
        return carry

    lax.fori_loop(0, tokens // blk, step, 0)
    d_scr[i, 1] = (dk_acc[...] * scale).astype(BF)
    d_scr[i, 2] = dv_acc[...].astype(BF)
    d_ref[0] = d_scr[i]
    start_all(d_copies(i))

    @pl.when(i == steps - 1)
    def _():
        for n in range(steps):
            wait_all(d_copies(n))
        wait_all(x_copies)


def attn_bwd(qkv, o, lse, g, kv, early, heads, blk):
    steps, _, hd, tokens = qkv.shape
    batch = steps // heads
    hbm = pl.BlockSpec(memory_space=pl.ANY)
    dma = pltpu.SemaphoreType.DMA
    row = lambda i: (i, 0, 0)
    return pl.pallas_call(
        functools.partial(attn_bwd_kernel, hd ** -0.5, blk, heads),
        grid=(steps,),
        in_specs=[pl.BlockSpec((1, 3, hd, tokens), lambda i: (i, 0, 0, 0)), pl.BlockSpec((1, hd, tokens), row), pl.BlockSpec((1, 1, tokens), row), hbm, hbm, hbm],
        out_specs=[pl.BlockSpec((1, 3, hd, tokens), lambda i: (i, 0, 0, 0)), hbm, hbm, hbm],
        out_shape=[jax.ShapeDtypeStruct(qkv.shape, BF), jax.ShapeDtypeStruct((batch, N_DEV * heads, 3, hd, blk), BF),
                   jax.ShapeDtypeStruct(kv.shape, BF), jax.ShapeDtypeStruct((N_DEV,) + early.shape, F32)],
        scratch_shapes=[pltpu.VMEM((steps, hd, tokens), BF), pltpu.VMEM(qkv.shape, BF), pltpu.VMEM((hd, tokens), F32), pltpu.VMEM((hd, tokens), F32),
                        dma((steps, N_DEV)), dma((steps, N_DEV)), dma((steps, N_DEV)), dma((steps, N_DEV)), dma((2, N_DEV)), dma((2, N_DEV))],
        cost_estimate=pl.CostEstimate(flops=10 * steps * hd * tokens * tokens, bytes_accessed=steps * hd * tokens * 20, transcendentals=steps * tokens * tokens),
        compiler_params=pltpu.CompilerParams(collective_id=2, has_side_effects=True, vmem_limit_bytes=56 << 20),
        name="attn_bwd",
    )(qkv, o, lse, g, kv, early)


def cross_fwd_kernel(scale, len_ref, q_ref, kv_ref, c_ref, p_ref):
    heads, slots = q_ref.shape[1], kv_ref.shape[5]
    blk = q_ref.shape[3]
    count = len_ref[pl.program_id(0)]
    ok = lax.broadcasted_iota(jnp.int32, (slots, blk), 0) < count
    for h in range(heads):
        s = dot00(kv_ref[h // 2, 0, h % 2, 0], q_ref[0, h]) * scale
        s = jnp.where(ok, s, MASK_FILL)
        p = jnp.exp(s - jnp.max(s, axis=0, keepdims=True))
        p = (p / jnp.sum(p, axis=0, keepdims=True)).astype(BF)
        p_ref[0, h] = p
        c_ref[0, h] = dot10(kv_ref[h // 2, 0, h % 2, 1], p).astype(BF)


def cross_specs(hd, blk, slots, per):
    q_spec = pl.BlockSpec((1, per, hd, blk), lambda b, i, n: (b, i, 0, 0))
    kv_spec = pl.BlockSpec((per // 2, 1, 2, 2, hd, slots), lambda b, i, n: (i, b, 0, 0, 0, 0))
    p_spec = pl.BlockSpec((1, per, slots, blk), lambda b, i, n: (b, i, 0, 0))
    return q_spec, kv_spec, p_spec


def cross_fwd(lens, q, kv, per=8):
    batch, heads, hd, blk = q.shape
    slots = kv.shape[5]
    q_spec, kv_spec, p_spec = cross_specs(hd, blk, slots, per)
    return pl.pallas_call(
        functools.partial(cross_fwd_kernel, hd ** -0.5),
        grid_spec=pltpu.PrefetchScalarGridSpec(num_scalar_prefetch=1, grid=(batch, heads // per), in_specs=[q_spec, kv_spec], out_specs=[q_spec, p_spec]),
        out_shape=[jax.ShapeDtypeStruct(q.shape, BF), jax.ShapeDtypeStruct((batch, heads, slots, blk), BF)],
        cost_estimate=pl.CostEstimate(flops=4 * batch * heads * hd * blk * slots * 8, bytes_accessed=batch * heads * blk * (hd * 4 + slots * 2), transcendentals=batch * heads * blk * slots),
        compiler_params=pltpu.CompilerParams(vmem_limit_bytes=32 << 20),
        name="cross_fwd",
    )(lens, q, kv)


def cross_bwd_kernel(scale, len_ref, q_ref, kv_ref, p_ref, g_ref, gq_ref, gkv_ref):
    heads = q_ref.shape[1]
    for h in range(heads):
        k, v = kv_ref[h // 2, 0, h % 2, 0], kv_ref[h // 2, 0, h % 2, 1]
        q, g, p = q_ref[0, h], g_ref[0, h], p_ref[0, h]
        dp = dot00(v, g)
        pf = p.astype(F32)
        delta = jnp.sum(dp * pf, axis=0, keepdims=True)
        ds = (pf * (dp - delta) * scale).astype(BF)
        gq_ref[0, h] = dot10(k, ds).astype(BF)
        gkv_ref[h // 2, 0, h % 2, 0] = dot11(q, ds).astype(BF)
        gkv_ref[h // 2, 0, h % 2, 1] = dot11(g, p).astype(BF)


def cross_bwd(lens, q, kv, prob, g, per=8):
    batch, heads, hd, blk = q.shape
    slots = kv.shape[5]
    q_spec, kv_spec, p_spec = cross_specs(hd, blk, slots, per)
    return pl.pallas_call(
        functools.partial(cross_bwd_kernel, hd ** -0.5),
        grid_spec=pltpu.PrefetchScalarGridSpec(num_scalar_prefetch=1, grid=(batch, heads // per), in_specs=[q_spec, kv_spec, p_spec, q_spec], out_specs=[q_spec, kv_spec]),
        out_shape=[jax.ShapeDtypeStruct(q.shape, BF), jax.ShapeDtypeStruct(kv.shape, BF)],
        cost_estimate=pl.CostEstimate(flops=8 * batch * heads * hd * blk * slots * 8, bytes_accessed=batch * heads * blk * (hd * 6 + slots * 2), transcendentals=0),
        compiler_params=pltpu.CompilerParams(vmem_limit_bytes=32 << 20),
        name="cross_bwd",
    )(lens, q, kv, prob, g)


def gather_rows(tensor, axes=TP):
    return lax.all_gather(tensor, axes, axis=0, tiled=True)


def scatter_rows(tensor, axes=TP):
    return lax.psum_scatter(tensor.astype(BF), axes, scatter_dimension=0, tiled=True)


def swap_y(tensor):
    return lax.ppermute(tensor, 'y', [(0, 1), (1, 0)])


def mlp_half(h2, g_mlp, w1_half, b1_half, w2_half):
    hidden = product('btd,fd->btf', h2, w1_half) + b1_half
    gelu_out, gelu_vjp = jax.vjp(gelu_tanh, hidden)
    gelu_out = gelu_out.astype(BF)
    g_hidden = gelu_vjp(product('btd,fd->btf', g_mlp, w2_half))[0]
    g_b_1 = jnp.sum(g_hidden, axis=(0, 1))
    g_hidden = g_hidden.astype(BF)
    g_h2 = product('btf,fd->btd', g_hidden, w1_half)
    part = product('btf,fd->btd', gelu_out, w2_half)
    return gelu_out, part, g_hidden, g_b_1, g_h2


def device_block(x_loc, y_loc, t_loc, len_loc, mod_table, w_qkv, b_qkv, w_o, b_o, w_q, b_q, w_kv, b_kv, w_co, b_co, w_1, b_1, w_2, b_2, g_loc):
    batch, n_loc, width = x_loc.shape
    heads_loc, head_dim = w_q.shape[1], w_q.shape[2]
    heads = heads_loc * N_DEV
    inner = heads * head_dim
    slots_loc = y_loc.shape[1]
    slots = slots_loc * N_DEV
    slots_pad = 128
    ffn_loc = w_1.shape[1]
    ffn = ffn_loc * N_DEV
    mod_rows = mod_table.astype(F32)[None] + t_loc.astype(F32).reshape(batch, 6, width)
    shift1, scale1, gate1, shift2, scale2, gate2 = [mod_rows[:, row_idx, None, :] for row_idx in range(6)]

    g_x2 = g_loc.astype(F32)
    g_mlp_f = g_x2 * gate2
    g_b_2 = jnp.sum(g_mlp_f, axis=(0, 1))
    g_mlp = g_mlp_f.astype(BF)

    normed1, inv_std1 = layer_norm(x_loc)
    h1 = (normed1 * (1.0 + scale1) + shift1).astype(BF)

    rows_loc = heads_loc * head_dim
    wqkv_t = w_qkv.transpose(1, 2, 0)
    wkv_t = w_kv.transpose(1, 2, 0)
    wq_t = w_q.transpose(1, 2, 0).reshape(rows_loc, width)
    small = jnp.concatenate([b_q.reshape(-1), b_1])
    small = jnp.pad(small, (0, width - small.shape[0]))[None]
    n_rows = batch * n_loc
    n_text = batch * slots_loc
    first = jnp.concatenate([h1.reshape(n_rows, width), y_loc.reshape(n_text, width), small, jnp.zeros((31 - n_text, width), BF)], axis=0)
    first = gather_rows(first[None])
    h1_all = first[:, :n_rows].reshape(N_DEV, batch, n_loc, width)
    y_all = first[:, n_rows:n_rows + n_text].reshape(N_DEV, batch, slots_loc, width).transpose(1, 0, 2, 3).reshape(batch, slots, width)
    y_all = jnp.pad(y_all, ((0, 0), (0, slots_pad - slots), (0, 0)))
    small_all = first[:, n_rows + n_text]
    bq_all = small_all[:, :rows_loc].reshape(inner)
    b1_all = small_all[:, rows_loc:rows_loc + ffn_loc].reshape(2, ffn // 2)
    b1_half = lax.dynamic_index_in_dim(b1_all, lax.axis_index('y'), keepdims=False)
    square = jnp.concatenate([w_o.reshape(rows_loc, width), wq_t, w_co.reshape(rows_loc, width)], axis=0)
    square = gather_rows(square[None])
    w1_half = gather_rows(w_1.T, ROW)
    w2_half = gather_rows(w_2, ROW)
    wqkv_all = gather_rows(wqkv_t.reshape(heads_loc * 3 * head_dim, width))

    tokens = N_DEV * n_loc
    qkv = (product('hed,jbtd->bhejt', wqkv_t, h1_all) + b_qkv[None, :, :, None, None]).astype(BF)
    qkv = qkv.reshape(batch * heads_loc, 3, head_dim, tokens)
    kv_t = (product('hed,bsd->bhes', wkv_t, y_all) + b_kv[None, :, :, None]).astype(BF)
    o_heads, lse, o_tok, kv_all = attn_fwd(qkv, kv_t.reshape(batch, heads_loc, 2, head_dim, slots_pad), heads_loc, n_loc)
    o_tok = o_tok.reshape(batch, inner, n_loc)
    g_mlp, square, o_tok = lax.optimization_barrier((g_mlp, square, o_tok))
    g_mlp_far = swap_y(g_mlp)
    wo_all, wq_all, wco_all = [square[:, n * rows_loc:(n + 1) * rows_loc].reshape(inner, width) for n in range(3)]

    attn_total = product('bet,ed->btd', o_tok, wo_all) + b_o
    x1 = (x_loc + gate1 * attn_total).astype(BF)
    q_cross = (product('ed,btd->bet', wq_all, x1) + bq_all[None, :, None]).astype(BF)
    q_cross = q_cross.reshape(batch, heads, head_dim, n_loc)
    cross_val, cross_prob = cross_fwd(len_loc, q_cross, kv_all)
    cross_rows = cross_val.reshape(batch, inner, n_loc)
    x2 = (x1 + (product('bet,ed->btd', cross_rows, wco_all) + b_co)).astype(BF)

    normed2, inv_std2 = layer_norm(x2)
    h2 = (normed2 * (1.0 + scale2) + shift2).astype(BF)
    own = mlp_half(h2, g_mlp, w1_half, b1_half, w2_half)
    h2_far = swap_y(h2)
    far = mlp_half(h2_far, g_mlp_far, w1_half, b1_half, w2_half)
    g_h2_far, gelu_own, g_hid_own = lax.optimization_barrier((far[4].astype(BF), own[0], own[2]))
    g_h2 = own[4] + swap_y(g_h2_far).astype(F32)
    part_far = swap_y(far[1].astype(BF))
    pair = lambda near, other: jnp.concatenate([near, other], axis=0)
    p_w_2 = product('btf,btd->fd', pair(gelu_own, far[0]), pair(g_mlp, g_mlp_far)).astype(BF)
    p_w_1 = product('btf,btd->fd', pair(g_hid_own, far[2]), pair(h2, h2_far)).astype(BF)
    g_h2, p_w_2, p_w_1, wqkv_all = lax.optimization_barrier((g_h2, p_w_2, p_w_1, wqkv_all))
    g_w_2 = scatter_rows(p_w_2, ROW)
    g_w_1 = scatter_rows(p_w_1, ROW).T
    g_b_1 = own[3] + far[3]
    g_shift2 = jnp.sum(g_h2, axis=(0, 1))
    g_scale2 = jnp.sum(g_h2 * normed2, axis=(0, 1))
    g_x2 = g_x2 + layer_norm_back(normed2, inv_std2, g_h2 * (1.0 + scale2))

    g_b_co = jnp.sum(g_x2, axis=(0, 1))
    g_cross = g_x2.astype(BF)
    p_w_co = product('bet,btd->ed', cross_rows, g_cross).astype(BF)
    g_cross_val = product('btd,ed->bet', g_cross, wco_all).astype(BF).reshape(batch, heads, head_dim, n_loc)
    g_q, g_kv = cross_bwd(len_loc, q_cross, kv_all, cross_prob, g_cross_val)
    g_q, part_far = lax.optimization_barrier((g_q, part_far))
    mlp_total = own[1] + part_far.astype(F32) + b_2
    x_out = (x2 + gate2 * mlp_total).astype(BF)
    g_gate2 = jnp.sum(g_loc.astype(F32) * mlp_total, axis=(0, 1))
    g_q = g_q.reshape(batch, inner, n_loc)
    g_b_q = jnp.sum(g_q.astype(F32), axis=(0, 2))
    p_w_q = product('bet,btd->ed', g_q, x1).astype(BF)
    g_x1 = g_x2 + product('bet,ed->btd', g_q, wq_all)
    g_gate1 = jnp.sum(g_x1 * attn_total, axis=(0, 1))
    g_attn_f = g_x1 * gate1
    g_b_o = jnp.sum(g_attn_f, axis=(0, 1))
    g_attn = g_attn_f.astype(BF)
    p_w_o = product('bet,btd->ed', o_tok, g_attn).astype(BF)
    g_o = product('btd,ed->bet', g_attn, wo_all).astype(BF).reshape(batch, heads, head_dim, n_loc)
    g_o, p_w_co, p_w_q, p_w_o = lax.optimization_barrier((g_o, p_w_co, p_w_q, p_w_o))
    g_w_co, g_w_q, g_w_o = scatter_rows(p_w_co), scatter_rows(p_w_q), scatter_rows(p_w_o)
    g_b_1 = jnp.where(lax.axis_index('y') == jnp.arange(2)[:, None], g_b_1[None], 0.0).reshape(ffn // width, width)
    early = jnp.stack([g_gate1, g_shift2, g_scale2, g_gate2, g_b_o, g_b_q, g_b_co, g_b_2])
    early = jnp.concatenate([early, g_b_1, jnp.zeros((16 - 8 - ffn // width, width), F32)], axis=0)
    g_qkv, g_qkv_tok, g_kv, early = attn_bwd(qkv, o_heads, lse, g_o, g_kv, early, heads_loc, n_loc)
    g_kv = jnp.sum(g_kv.astype(F32), axis=0).reshape(batch, heads_loc, 2 * head_dim, slots_pad)
    g_b_kv = jnp.sum(g_kv, axis=(0, 3))
    g_kv = g_kv.astype(BF)
    g_y = product('bhes,hed->bsd', g_kv, wkv_t)[:, :slots].astype(BF)
    g_y = g_y.reshape(batch, N_DEV, slots_loc, width).transpose(1, 0, 2, 3).reshape(N_DEV, n_text, width)
    g_y = jnp.pad(g_y, ((0, 0), (0, 32 - n_text), (0, 0)))
    g_w_kv = product('bhes,bsd->hed', g_kv, y_all).astype(BF).transpose(2, 0, 1)
    g_h1 = product('bet,ed->btd', g_qkv_tok.reshape(batch, 3 * inner, n_loc), wqkv_all)
    g_rows = g_qkv.reshape(batch, heads_loc, 3 * head_dim, N_DEV, n_loc)
    g_b_qkv = jnp.sum(g_rows.astype(F32), axis=(0, 3, 4))
    g_w_qkv = product('bhejt,jbtd->hed', g_rows, h1_all).astype(BF).transpose(2, 0, 1)
    g_x = g_x1 + layer_norm_back(normed1, inv_std1, g_h1 * (1.0 + scale1))
    late = jnp.stack([jnp.sum(g_h1, axis=(0, 1)), jnp.sum(g_h1 * normed1, axis=(0, 1))])
    late = jnp.pad(late, ((0, 6), (0, 0)))
    late, g_w_2, g_w_1 = lax.optimization_barrier((late, g_w_2, g_w_1))
    g_y, late = late_exchange(g_y, late)
    g_y = jnp.sum(g_y.astype(F32), axis=0)[:n_text].reshape(batch, slots_loc, width).astype(BF)
    late = jnp.sum(late, axis=0)
    early = jnp.sum(early, axis=0)
    me = my_index()
    g_b_q = lax.dynamic_slice(early[5], (me * heads_loc * head_dim,), (heads_loc * head_dim,)).reshape(heads_loc, head_dim)
    g_b_1 = lax.dynamic_slice(early[8:8 + ffn // width].reshape(ffn), (me * ffn_loc,), (ffn_loc,))

    return (x_out, g_x.astype(BF), g_y, jnp.concatenate([late[:2], early[:4]], axis=0), g_w_qkv, g_b_qkv.astype(BF), g_w_o.reshape(heads_loc, head_dim, width), early[4].astype(BF), g_w_q.reshape(heads_loc, head_dim, width).transpose(2, 0, 1), g_b_q.astype(BF), g_w_kv, g_b_kv.astype(BF), g_w_co.reshape(heads_loc, head_dim, width), early[6].astype(BF), g_w_1, g_b_1.astype(BF), g_w_2, early[7].astype(BF))


def solution(mesh):
    mesh = jax.sharding.Mesh(mesh.devices.reshape(-1, 2, 2, 2), ('dp',) + TP)
    token_spec = P('dp', TP, None)
    group_rows = ('dp',) + TP
    in_specs = (token_spec, token_spec, P('dp', None), P('dp'), P(None, None), P(None, TP, None), P(TP, None), P(TP, None, None), P(None), P(None, TP, None), P(TP, None), P(None, TP, None), P(TP, None), P(TP, None, None), P(None), P(None, TP), P(TP), P(TP, None), P(None), token_spec)
    out_specs = (token_spec, token_spec, token_spec, P('dp', None), P('dp', TP, None), P(group_rows, None), P(group_rows, None, None), P('dp'), P('dp', TP, None), P(group_rows, None), P('dp', TP, None), P(group_rows, None), P(group_rows, None, None), P('dp'), P('dp', TP), P(group_rows), P(group_rows, None), P('dp'))
    return jax.shard_map(device_block, mesh=mesh, in_specs=in_specs, out_specs=out_specs, check_vma=False)
```

```python
import functools
import math

import jax
import jax.numpy as jnp
from jax import lax
from jax.experimental import pallas as pl
from jax.experimental.pallas import tpu as pltpu
from jax.sharding import PartitionSpec as P


LN_EPS = 1e-6
MASK_FILL = -1e30
N_DEV = 8
TP = ('y', 'x', 'c')
ROW = ('x', 'c')
UNROLL = 1
LOG2E = math.log2(math.e)
BF = jnp.bfloat16
F32 = jnp.float32


def product(form, lhs, rhs):
    return jnp.einsum(form, lhs, rhs, preferred_element_type=F32)


def layer_norm(tensor):
    tensor = tensor.astype(F32)
    centered = tensor - jnp.mean(tensor, axis=-1, keepdims=True)
    inv_std = lax.rsqrt(jnp.mean(centered * centered, axis=-1, keepdims=True) + LN_EPS)
    return centered * inv_std, inv_std


def layer_norm_back(normed, inv_std, g_normed):
    mean_g = jnp.mean(g_normed, axis=-1, keepdims=True)
    mean_gn = jnp.mean(g_normed * normed, axis=-1, keepdims=True)
    return inv_std * (g_normed - mean_g - normed * mean_gn)


def gelu_tanh(tensor):
    return jax.nn.gelu(tensor, approximate=True)


def dot00(lhs, rhs):
    return lax.dot_general(lhs, rhs, (((0,), (0,)), ((), ())), preferred_element_type=F32)


def dot10(lhs, rhs):
    return lax.dot_general(lhs, rhs, (((1,), (0,)), ((), ())), preferred_element_type=F32)


def dot11(lhs, rhs):
    return lax.dot_general(lhs, rhs, (((1,), (1,)), ((), ())), preferred_element_type=F32)


def my_index():
    return lax.axis_index('y') * 4 + lax.axis_index('x') * 2 + lax.axis_index('c')


def device(index):
    return {'y': index // 4, 'x': (index // 2) % 2, 'c': index % 2}


def entry_barrier(me):
    barrier = pltpu.get_barrier_semaphore()
    for k in range(1, N_DEV):
        pl.semaphore_signal(barrier, inc=1, device_id=device(me ^ k), device_id_type=pl.DeviceIdType.MESH)
    pl.semaphore_wait(barrier, N_DEV - 1)


def block_copy(src, dst, send_sem, recv_sem, peer, k):
    if k == 0:
        return pltpu.make_async_copy(src, dst, recv_sem)
    return pltpu.make_async_remote_copy(src_ref=src, dst_ref=dst, send_sem=send_sem, recv_sem=recv_sem, device_id=device(peer), device_id_type=pl.DeviceIdType.MESH)


def start_all(copies):
    for copy in copies:
        copy.start()


def wait_all(copies):
    for copy in copies:
        copy.wait()


def block_at(index, blk):
    return pl.ds(pl.multiple_of(index * blk, blk), blk)


def attn_fwd_kernel(scale, blk, heads, qkv_ref, kv_ref, o_ref, lse_ref, tok_ref, kv_out, o_scr, send, recv, kv_send, kv_recv):
    i = pl.program_id(0)
    last = pl.num_programs(0) - 1
    tokens = o_ref.shape[2]
    factor = scale * LOG2E
    me = my_index()

    def o_copies(step):
        return [block_copy(o_scr.at[step, :, block_at(me ^ k, blk)], tok_ref.at[step // heads, me * heads + step % heads], send.at[step, k], recv.at[step, k], me ^ k, k) for k in range(N_DEV)]

    kv_copies = [block_copy(kv_ref, kv_out.at[me], kv_send.at[k], kv_recv.at[k], me ^ k, k) for k in range(N_DEV)]

    @pl.when(i == 0)
    def _():
        entry_barrier(me)
        start_all(kv_copies)

    def step(j, carry):
        cols = block_at(j, blk)
        s = dot00(qkv_ref[0, 1], qkv_ref[0, 0, :, cols])
        top = jnp.max(s, axis=0, keepdims=True) * factor
        p = jnp.exp2(s * factor - top)
        total = jnp.sum(p, axis=0, keepdims=True)
        o = dot10(qkv_ref[0, 2], p.astype(BF))
        o_scr[i, :, cols] = (o / total).astype(BF)
        lse_ref[0, :, cols] = top + jnp.log2(total)
        return carry

    lax.fori_loop(0, tokens // blk, step, 0, unroll=UNROLL)
    o_ref[0] = o_scr[i]
    start_all(o_copies(i))

    @pl.when(i == last)
    def _():
        for n in range(o_scr.shape[0]):
            wait_all(o_copies(n))
        wait_all(kv_copies)


def attn_fwd(qkv, kv, heads, blk):
    steps, _, hd, tokens = qkv.shape
    batch = steps // heads
    hbm = pl.BlockSpec(memory_space=pl.ANY)
    dma = pltpu.SemaphoreType.DMA
    return pl.pallas_call(
        functools.partial(attn_fwd_kernel, hd ** -0.5, blk, heads),
        grid=(steps,),
        in_specs=[pl.BlockSpec((1, 3, hd, tokens), lambda i: (i, 0, 0, 0)), hbm],
        out_specs=[pl.BlockSpec((1, hd, tokens), lambda i: (i, 0, 0)), pl.BlockSpec((1, 1, tokens), lambda i: (i, 0, 0)), hbm, hbm],
        out_shape=[jax.ShapeDtypeStruct((steps, hd, tokens), BF), jax.ShapeDtypeStruct((steps, 1, tokens), F32),
                   jax.ShapeDtypeStruct((batch, N_DEV * heads, hd, blk), BF), jax.ShapeDtypeStruct((N_DEV,) + kv.shape, BF)],
        scratch_shapes=[pltpu.VMEM((steps, hd, tokens), BF), dma((steps, N_DEV)), dma((steps, N_DEV)), dma((N_DEV,)), dma((N_DEV,))],
        cost_estimate=pl.CostEstimate(flops=4 * steps * hd * tokens * tokens, bytes_accessed=steps * hd * tokens * 8, transcendentals=steps * tokens * tokens),
        compiler_params=pltpu.CompilerParams(collective_id=1, has_side_effects=True, vmem_limit_bytes=48 << 20),
        name="attn_fwd",
    )(qkv, kv)


def attn_bwd_kernel(scale, blk, heads, qkv_ref, o_ref, lse_ref, g_ref, *refs):
    rows, (d_ref, tok_ref, early_out, g_scr, d_scr, early_scr, dk_acc, dv_acc, g_send, g_recv, d_send, d_recv, x_send, x_recv) = refs[:-14], refs[-14:]
    i = pl.program_id(0)
    steps = d_scr.shape[0]
    tokens = o_ref.shape[2]
    factor = scale * LOG2E
    me = my_index()

    def g_copies(step):
        return [block_copy(g_ref.at[step // heads, (me ^ k) * heads + step % heads], g_scr.at[step, :, block_at(me, blk)], g_send.at[step, k], g_recv.at[step, k], me ^ k, k) for k in range(N_DEV)]

    def d_copies(step):
        return [block_copy(d_scr.at[step, :, :, block_at(me ^ k, blk)], tok_ref.at[step // heads, me * heads + step % heads], d_send.at[step, k], d_recv.at[step, k], me ^ k, k) for k in range(N_DEV)]

    x_copies = [block_copy(early_scr, early_out.at[me], x_send.at[k], x_recv.at[k], me ^ k, k) for k in range(N_DEV)]

    @pl.when(i == 0)
    def _():
        entry_barrier(me)
        for n in range(steps):
            start_all(g_copies(n))
        early_scr[...] = jnp.zeros_like(early_scr)
        place = 0
        for row in rows:
            early_scr[place:place + row.shape[0], :] = row[...]
            place += row.shape[0]

    wait_all(g_copies(i))
    dk_acc[...] = jnp.zeros_like(dk_acc)
    dv_acc[...] = jnp.zeros_like(dv_acc)

    def step(j, carry):
        cols = block_at(j, blk)
        q = qkv_ref[0, 0, :, cols]
        g = g_scr[i, :, cols]
        delta = jnp.sum(g.astype(F32) * o_ref[0, :, cols].astype(F32), axis=0, keepdims=True)
        s = dot00(qkv_ref[0, 1], q)
        p = jnp.exp2(s * factor - lse_ref[0, :, cols])
        dp = dot00(qkv_ref[0, 2], g)
        ds = (p * (dp - delta)).astype(BF)
        dv_acc[...] += dot11(g, p.astype(BF))
        dk_acc[...] += dot11(q, ds)
        d_scr[i, 0, :, cols] = (dot10(qkv_ref[0, 1], ds) * scale).astype(BF)
        return carry

    lax.fori_loop(0, tokens // blk, step, 0, unroll=UNROLL)
    d_scr[i, 1] = (dk_acc[...] * scale).astype(BF)
    d_scr[i, 2] = dv_acc[...].astype(BF)
    d_ref[0] = d_scr[i]
    start_all(d_copies(i))

    @pl.when(i == 0)
    def _():
        start_all(x_copies)

    @pl.when(i == steps - 1)
    def _():
        for n in range(steps):
            wait_all(d_copies(n))
        wait_all(x_copies)


def attn_bwd(qkv, o, lse, g, early, heads, blk):
    steps, _, hd, tokens = qkv.shape
    batch = steps // heads
    hbm = pl.BlockSpec(memory_space=pl.ANY)
    dma = pltpu.SemaphoreType.DMA
    row = lambda i: (i, 0, 0)
    return pl.pallas_call(
        functools.partial(attn_bwd_kernel, hd ** -0.5, blk, heads),
        grid=(steps,),
        in_specs=[pl.BlockSpec((1, 3, hd, tokens), lambda i: (i, 0, 0, 0)), pl.BlockSpec((1, hd, tokens), row), pl.BlockSpec((1, 1, tokens), row), hbm] + [pl.BlockSpec(part.shape, lambda i: (0, 0)) for part in early],
        out_specs=[pl.BlockSpec((1, 3, hd, tokens), lambda i: (i, 0, 0, 0)), hbm, hbm],
        out_shape=[jax.ShapeDtypeStruct(qkv.shape, BF), jax.ShapeDtypeStruct((batch, N_DEV * heads, 3, hd, blk), BF),
                   jax.ShapeDtypeStruct((N_DEV, 16, early[0].shape[1]), F32)],
        scratch_shapes=[pltpu.VMEM((steps, hd, tokens), BF), pltpu.VMEM(qkv.shape, BF), pltpu.VMEM((16, early[0].shape[1]), F32), pltpu.VMEM((hd, tokens), F32), pltpu.VMEM((hd, tokens), F32),
                        dma((steps, N_DEV)), dma((steps, N_DEV)), dma((steps, N_DEV)), dma((steps, N_DEV)), dma((N_DEV,)), dma((N_DEV,))],
        cost_estimate=pl.CostEstimate(flops=10 * steps * hd * tokens * tokens, bytes_accessed=steps * hd * tokens * 20, transcendentals=steps * tokens * tokens),
        compiler_params=pltpu.CompilerParams(collective_id=2, has_side_effects=True, vmem_limit_bytes=56 << 20),
        name="attn_bwd",
    )(qkv, o, lse, g, *early)


def qkv_kernel(w_ref, b_ref, h_ref, out_ref):
    out_ref[0] = (dot11(w_ref[...], h_ref[0]) + b_ref[...]).astype(BF)


def qkv_project(w, bias, first, batch, blk):
    rows, width = w.shape
    return pl.pallas_call(
        qkv_kernel,
        grid=(batch, N_DEV),
        in_specs=[pl.BlockSpec((rows, width), lambda b, j: (0, 0)), pl.BlockSpec((rows, 1), lambda b, j: (0, 0)), pl.BlockSpec((1, blk, width), lambda b, j: (j, b, 0))],
        out_specs=pl.BlockSpec((1, rows, blk), lambda b, j: (b, 0, j)),
        out_shape=jax.ShapeDtypeStruct((batch, rows, N_DEV * blk), BF),
        cost_estimate=pl.CostEstimate(flops=2 * rows * width * batch * N_DEV * blk, bytes_accessed=2 * batch * N_DEV * blk * (rows + width), transcendentals=0),
        compiler_params=pltpu.CompilerParams(vmem_limit_bytes=24 << 20),
        name="qkv_project",
    )(w, bias, first)


def qkv_grad_kernel(g_ref, h_ref, parts, whole, w_ref, b_ref, parts_out, whole_out, w_acc, b_acc, send, recv):
    n = pl.program_id(0)
    me = my_index()
    copies = []
    for k in range(N_DEV):
        copies.append(block_copy(whole, whole_out.at[me], send.at[0, k], recv.at[0, k], me ^ k, k))
        copies.append(block_copy(parts.at[me ^ k], parts_out.at[me], send.at[1, k], recv.at[1, k], me ^ k, k))

    @pl.when(n == 0)
    def _():
        entry_barrier(me)
        start_all(copies)
        w_acc[...] = jnp.zeros_like(w_acc)
        b_acc[...] = jnp.zeros_like(b_acc)

    g = g_ref[0]
    w_acc[...] += dot10(g, h_ref[0])
    b_acc[...] += g.astype(F32)

    @pl.when(n == pl.num_programs(0) - 1)
    def _():
        w_ref[...] = w_acc[...].astype(BF)
        b_ref[...] = jnp.sum(b_acc[...], axis=1, keepdims=True)
        wait_all(copies)


def qkv_grad(g, first, parts, whole, blk):
    batch, rows, tokens = g.shape
    width = first.shape[2]
    hbm = pl.BlockSpec(memory_space=pl.ANY)
    dma = pltpu.SemaphoreType.DMA
    return pl.pallas_call(
        qkv_grad_kernel,
        grid=(batch * N_DEV,),
        in_specs=[pl.BlockSpec((1, rows, blk), lambda n: (n // N_DEV, 0, n % N_DEV)), pl.BlockSpec((1, blk, width), lambda n: (n % N_DEV, n // N_DEV, 0)), hbm, hbm],
        out_specs=[pl.BlockSpec((rows, width), lambda n: (0, 0)), pl.BlockSpec((rows, 1), lambda n: (0, 0)), hbm, hbm],
        out_shape=[jax.ShapeDtypeStruct((rows, width), BF), jax.ShapeDtypeStruct((rows, 1), F32),
                   jax.ShapeDtypeStruct(parts.shape, parts.dtype), jax.ShapeDtypeStruct((N_DEV,) + whole.shape, whole.dtype)],
        scratch_shapes=[pltpu.VMEM((rows, width), F32), pltpu.VMEM((rows, blk), F32), dma((2, N_DEV)), dma((2, N_DEV))],
        cost_estimate=pl.CostEstimate(flops=2 * rows * width * batch * tokens, bytes_accessed=2 * batch * tokens * (rows + width), transcendentals=0),
        compiler_params=pltpu.CompilerParams(collective_id=3, has_side_effects=True, vmem_limit_bytes=24 << 20),
        name="qkv_grad",
    )(g, first, parts, whole)


def cross_fwd_kernel(scale, len_ref, q_ref, kv_ref, c_ref, p_ref):
    heads, slots = q_ref.shape[1], kv_ref.shape[5]
    blk = q_ref.shape[3]
    count = len_ref[pl.program_id(0)]
    ok = lax.broadcasted_iota(jnp.int32, (slots, blk), 0) < count
    for h in range(heads):
        s = dot00(kv_ref[h // 2, 0, h % 2, 0], q_ref[0, h]) * scale
        s = jnp.where(ok, s, MASK_FILL)
        p = jnp.exp(s - jnp.max(s, axis=0, keepdims=True))
        p = (p / jnp.sum(p, axis=0, keepdims=True)).astype(BF)
        p_ref[0, h] = p
        c_ref[0, h] = dot10(kv_ref[h // 2, 0, h % 2, 1], p).astype(BF)


def cross_specs(hd, blk, slots, per):
    q_spec = pl.BlockSpec((1, per, hd, blk), lambda b, i, n: (b, i, 0, 0))
    kv_spec = pl.BlockSpec((per // 2, 1, 2, 2, hd, slots), lambda b, i, n: (i, b, 0, 0, 0, 0))
    p_spec = pl.BlockSpec((1, per, slots, blk), lambda b, i, n: (b, i, 0, 0))
    return q_spec, kv_spec, p_spec


def cross_fwd(lens, q, kv, per=8):
    batch, heads, hd, blk = q.shape
    slots = kv.shape[5]
    q_spec, kv_spec, p_spec = cross_specs(hd, blk, slots, per)
    return pl.pallas_call(
        functools.partial(cross_fwd_kernel, hd ** -0.5),
        grid_spec=pltpu.PrefetchScalarGridSpec(num_scalar_prefetch=1, grid=(batch, heads // per), in_specs=[q_spec, kv_spec], out_specs=[q_spec, p_spec]),
        out_shape=[jax.ShapeDtypeStruct(q.shape, BF), jax.ShapeDtypeStruct((batch, heads, slots, blk), BF)],
        cost_estimate=pl.CostEstimate(flops=4 * batch * heads * hd * blk * slots * 8, bytes_accessed=batch * heads * blk * (hd * 4 + slots * 2), transcendentals=batch * heads * blk * slots),
        compiler_params=pltpu.CompilerParams(vmem_limit_bytes=32 << 20),
        name="cross_fwd",
    )(lens, q, kv)


def cross_bwd_kernel(scale, len_ref, q_ref, kv_ref, p_ref, g_ref, gq_ref, gkv_ref):
    heads = q_ref.shape[1]
    for h in range(heads):
        k, v = kv_ref[h // 2, 0, h % 2, 0], kv_ref[h // 2, 0, h % 2, 1]
        q, g, p = q_ref[0, h], g_ref[0, h], p_ref[0, h]
        dp = dot00(v, g)
        pf = p.astype(F32)
        delta = jnp.sum(dp * pf, axis=0, keepdims=True)
        ds = (pf * (dp - delta) * scale).astype(BF)
        gq_ref[0, h] = dot10(k, ds).astype(BF)
        gkv_ref[h // 2, 0, h % 2, 0] = dot11(q, ds).astype(BF)
        gkv_ref[h // 2, 0, h % 2, 1] = dot11(g, p).astype(BF)


def cross_bwd(lens, q, kv, prob, g, per=8):
    batch, heads, hd, blk = q.shape
    slots = kv.shape[5]
    q_spec, kv_spec, p_spec = cross_specs(hd, blk, slots, per)
    return pl.pallas_call(
        functools.partial(cross_bwd_kernel, hd ** -0.5),
        grid_spec=pltpu.PrefetchScalarGridSpec(num_scalar_prefetch=1, grid=(batch, heads // per), in_specs=[q_spec, kv_spec, p_spec, q_spec], out_specs=[q_spec, kv_spec]),
        out_shape=[jax.ShapeDtypeStruct(q.shape, BF), jax.ShapeDtypeStruct(kv.shape, BF)],
        cost_estimate=pl.CostEstimate(flops=8 * batch * heads * hd * blk * slots * 8, bytes_accessed=batch * heads * blk * (hd * 6 + slots * 2), transcendentals=0),
        compiler_params=pltpu.CompilerParams(vmem_limit_bytes=32 << 20),
        name="cross_bwd",
    )(lens, q, kv, prob, g)


def gather_rows(tensor, axes=TP):
    return lax.all_gather(tensor, axes, axis=0, tiled=True)


def scatter_rows(tensor, axes=TP):
    return lax.psum_scatter(tensor.astype(BF), axes, scatter_dimension=0, tiled=True)


def swap(tensor, axis):
    return lax.ppermute(tensor, axis, [(0, 1), (1, 0)])


def swap_y(tensor):
    return swap(tensor, 'y')


def row_reduce(rows):
    grid = rows.reshape(2, 2, -1, rows.shape[1])
    core = lax.axis_index('c')
    other = swap(lax.dynamic_index_in_dim(grid, 1 - core, 1, keepdims=False), 'c')
    return (lax.dynamic_index_in_dim(grid, core, 1, keepdims=False).astype(F32) + other.astype(F32)).astype(BF)


def row_finish(pair):
    place = lax.axis_index('x')
    other = swap(lax.dynamic_index_in_dim(pair, 1 - place, 0, keepdims=False), 'x')
    return (lax.dynamic_index_in_dim(pair, place, 0, keepdims=False).astype(F32) + other.astype(F32)).astype(BF)


def mlp_hidden(h2, w1_half, b1_half):
    hidden = product('btd,fd->btf', h2, w1_half) + b1_half
    gelu_out, gelu_vjp = jax.vjp(gelu_tanh, hidden)
    return gelu_out.astype(BF), gelu_vjp


def mlp_rest(gelu_out, gelu_vjp, g_mlp, w1_half, w2_half, name):
    g_hidden = gelu_vjp(product('btd,fd->btf', g_mlp, w2_half))[0]
    g_b_1 = jnp.sum(g_hidden, axis=(0, 1))
    g_hidden = g_hidden.astype(BF)
    g_h2 = product('btf,fd->btd', g_hidden, w1_half)
    part = product('btf,fd->btd', gelu_out, w2_half)
    part = part if name == 'own' else part.astype(BF)
    return gelu_out, part, g_hidden, g_b_1, g_h2


def device_block(x_loc, y_loc, t_loc, len_loc, mod_table, w_qkv, b_qkv, w_o, b_o, w_q, b_q, w_kv, b_kv, w_co, b_co, w_1, b_1, w_2, b_2, g_loc):
    batch, n_loc, width = x_loc.shape
    heads_loc, head_dim = w_q.shape[1], w_q.shape[2]
    heads = heads_loc * N_DEV
    inner = heads * head_dim
    slots_loc = y_loc.shape[1]
    slots = slots_loc * N_DEV
    slots_pad = 128
    ffn_loc = w_1.shape[1]
    ffn = ffn_loc * N_DEV
    mod_rows = mod_table.astype(F32)[None] + t_loc.astype(F32).reshape(batch, 6, width)
    shift1, scale1, gate1, shift2, scale2, gate2 = [mod_rows[:, row_idx, None, :] for row_idx in range(6)]

    g_x2 = g_loc.astype(F32)
    g_mlp_f = g_x2 * gate2
    g_b_2 = jnp.sum(g_mlp_f, axis=(0, 1))
    g_mlp = g_mlp_f.astype(BF)

    normed1, inv_std1 = layer_norm(x_loc)
    h1 = (normed1 * (1.0 + scale1) + shift1).astype(BF)

    rows_loc = heads_loc * head_dim
    wqkv_t = w_qkv.transpose(1, 2, 0)
    wkv_t = w_kv.transpose(1, 2, 0)
    wq_t = w_q.transpose(1, 2, 0).reshape(rows_loc, width)
    small = jnp.concatenate([b_q.reshape(-1), b_1])
    small = jnp.pad(small, (0, width - small.shape[0]))[None]
    n_rows = batch * n_loc
    n_text = batch * slots_loc
    first = jnp.concatenate([h1.reshape(n_rows, width), y_loc.reshape(n_text, width), small, jnp.zeros((31 - n_text, width), BF)], axis=0)
    first = gather_rows(first[None])
    y_all = first[:, n_rows:n_rows + n_text].reshape(N_DEV, batch, slots_loc, width).transpose(1, 0, 2, 3).reshape(batch, slots, width)
    y_all = jnp.pad(y_all, ((0, 0), (0, slots_pad - slots), (0, 0)))
    small_all = first[:, n_rows + n_text]
    bq_all = small_all[:, :rows_loc].reshape(inner)
    b1_all = small_all[:, rows_loc:rows_loc + ffn_loc]
    b1_half = lax.dynamic_index_in_dim(b1_all.reshape(2, ffn // 2), lax.axis_index('y'), keepdims=False)
    square = jnp.concatenate([w_o.reshape(rows_loc, width), wq_t, w_co.reshape(rows_loc, width)], axis=0)
    square = gather_rows(square[None])
    w1_half = gather_rows(w_1.T, ROW)
    w2_half = gather_rows(w_2, ROW)
    wqkv_all = gather_rows(wqkv_t.reshape(heads_loc * 3 * head_dim, width))

    tokens = N_DEV * n_loc
    qkv_rows = heads_loc * 3 * head_dim
    qkv = qkv_project(wqkv_t.reshape(qkv_rows, width), b_qkv.astype(F32).reshape(qkv_rows, 1), first, batch, n_loc)
    qkv = qkv.reshape(batch * heads_loc, 3, head_dim, tokens)
    kv_t = (product('hed,bsd->bhes', wkv_t, y_all) + b_kv[None, :, :, None]).astype(BF)
    o_heads, lse, o_tok, kv_all = attn_fwd(qkv, kv_t.reshape(batch, heads_loc, 2, head_dim, slots_pad), heads_loc, n_loc)
    o_tok = o_tok.reshape(batch, inner, n_loc)
    square, o_tok, g_mlp = lax.optimization_barrier((square, o_tok, g_mlp))
    g_mlp_far = swap_y(g_mlp)
    wo_all, wq_all, wco_all = [square[:, n * rows_loc:(n + 1) * rows_loc].reshape(inner, width) for n in range(3)]

    attn_total = product('bet,ed->btd', o_tok, wo_all) + b_o
    x1 = (x_loc + gate1 * attn_total).astype(BF)
    q_cross = (product('ed,btd->bet', wq_all, x1) + bq_all[None, :, None]).astype(BF)
    q_cross = q_cross.reshape(batch, heads, head_dim, n_loc)
    cross_val, cross_prob = cross_fwd(len_loc, q_cross, kv_all)
    cross_rows = cross_val.reshape(batch, inner, n_loc)
    x2 = (x1 + (product('bet,ed->btd', cross_rows, wco_all) + b_co)).astype(BF)

    normed2, inv_std2 = layer_norm(x2)
    h2 = (normed2 * (1.0 + scale2) + shift2).astype(BF)
    gelu_own, vjp_own = mlp_hidden(h2, w1_half, b1_half)
    h2_far = swap_y(h2)
    gelu_far, vjp_far = mlp_hidden(h2_far, w1_half, b1_half)
    w2_half, gelu_own, gelu_far = lax.optimization_barrier((w2_half, gelu_own, gelu_far))
    own = mlp_rest(gelu_own, vjp_own, g_mlp, w1_half, w2_half, 'own')
    far = mlp_rest(gelu_far, vjp_far, g_mlp_far, w1_half, w2_half, 'far')
    g_h2_far, gelu_own, g_hid_own = far[4].astype(BF), own[0], own[2]
    g_h2_far = swap_y(g_h2_far)
    pair = lambda near, other: jnp.concatenate([near, other], axis=0)
    p_w_2 = product('btf,btd->fd', pair(gelu_own, far[0]), pair(g_mlp, g_mlp_far)).astype(BF)
    p_w_2 = row_reduce(p_w_2)
    p_w_1 = product('btf,btd->fd', pair(g_hid_own, far[2]), pair(h2, h2_far)).astype(BF)
    p_w_1 = row_reduce(p_w_1)
    part_own, part_far = own[1], far[1]
    g_h2_far, part_own, part_far, _, _ = lax.optimization_barrier((g_h2_far, part_own, part_far, p_w_2, p_w_1))
    g_h2 = own[4] + g_h2_far.astype(F32)
    part_far = swap_y(part_far)
    g_w_2 = row_finish(p_w_2)
    g_w_1 = row_finish(p_w_1).T
    g_b_1 = own[3] + far[3]
    g_shift2 = jnp.sum(g_h2, axis=(0, 1))
    g_scale2 = jnp.sum(g_h2 * normed2, axis=(0, 1))
    g_x2 = g_x2 + layer_norm_back(normed2, inv_std2, g_h2 * (1.0 + scale2))

    g_b_co = jnp.sum(g_x2, axis=(0, 1))
    g_cross = g_x2.astype(BF)
    p_w_co = product('bet,btd->ed', cross_rows, g_cross).astype(BF)
    g_cross_val = product('btd,ed->bet', g_cross, wco_all).astype(BF).reshape(batch, heads, head_dim, n_loc)
    g_cross_val, wqkv_all = lax.optimization_barrier((g_cross_val, wqkv_all))
    g_q, g_kv = cross_bwd(len_loc, q_cross, kv_all, cross_prob, g_cross_val)
    g_kv = scatter_rows(g_kv)
    g_q = g_q.reshape(batch, inner, n_loc)
    g_b_q = jnp.sum(g_q.astype(F32), axis=(0, 2))
    p_w_q = product('bet,btd->ed', g_q, x1).astype(BF)
    g_x1 = g_x2 + product('bet,ed->btd', g_q, wq_all)
    g_gate1 = jnp.sum(g_x1 * attn_total, axis=(0, 1))
    g_attn_f = g_x1 * gate1
    g_b_o = jnp.sum(g_attn_f, axis=(0, 1))
    g_attn = g_attn_f.astype(BF)
    p_w_o = product('bet,btd->ed', o_tok, g_attn).astype(BF)
    g_o = product('btd,ed->bet', g_attn, wo_all).astype(BF).reshape(batch, heads, head_dim, n_loc)
    g_w_co, g_w_q, g_w_o = scatter_rows(p_w_co), scatter_rows(p_w_q), scatter_rows(p_w_o)
    g_o, _, _, _ = lax.optimization_barrier((g_o, p_w_co, p_w_q, p_w_o))
    g_b_1 = jnp.where(lax.axis_index('y') == jnp.arange(2)[:, None], g_b_1[None], 0.0).reshape(ffn // width, width)
    early = [row[None] for row in (g_gate1, g_shift2, g_scale2, g_b_o, g_b_q, g_b_co, g_b_2)] + [g_b_1]
    g_qkv, g_qkv_tok, early = attn_bwd(qkv, o_heads, lse, g_o, early, heads_loc, n_loc)
    g_qkv_tok, part_far = lax.optimization_barrier((g_qkv_tok, part_far))
    g_kv, g_qkv_tok = lax.optimization_barrier((g_kv, g_qkv_tok))
    g_kv = g_kv.astype(F32).reshape(batch, heads_loc, 2 * head_dim, slots_pad)
    g_b_kv = jnp.sum(g_kv, axis=(0, 3))
    g_kv = g_kv.astype(BF)
    g_y = product('bhes,hed->bsd', g_kv, wkv_t)[:, :slots].astype(BF)
    g_y = g_y.reshape(batch, N_DEV, slots_loc, width).transpose(1, 0, 2, 3).reshape(N_DEV, n_text, width)
    g_y = jnp.pad(g_y, ((0, 0), (0, 32 - n_text), (0, 0)))
    g_w_kv = product('bhes,bsd->hed', g_kv, y_all).astype(BF).transpose(2, 0, 1)
    g_h1 = product('bet,ed->btd', g_qkv_tok.reshape(batch, 3 * inner, n_loc), wqkv_all)
    g_x = g_x1 + layer_norm_back(normed1, inv_std1, g_h1 * (1.0 + scale1))
    mlp_total = part_own + part_far.astype(F32) + b_2
    x_out = (x2 + gate2 * mlp_total).astype(BF)
    g_gate2 = jnp.sum(g_loc.astype(F32) * mlp_total, axis=(0, 1))
    late = jnp.stack([jnp.sum(g_h1, axis=(0, 1)), jnp.sum(g_h1 * normed1, axis=(0, 1)), g_gate2])
    late = jnp.pad(late, ((0, 5), (0, 0)))
    g_w_qkv, g_b_qkv, g_y, late = qkv_grad(g_qkv.reshape(batch, qkv_rows, tokens), first, g_y, late, n_loc)
    g_w_qkv = g_w_qkv.reshape(heads_loc, 3 * head_dim, width).transpose(2, 0, 1)
    g_b_qkv = g_b_qkv.reshape(heads_loc, 3 * head_dim)
    g_y = jnp.sum(g_y.astype(F32), axis=0)[:n_text].reshape(batch, slots_loc, width).astype(BF)
    late = jnp.sum(late, axis=0)
    early = jnp.sum(early, axis=0)
    me = my_index()
    g_b_q = lax.dynamic_slice(early[4], (me * heads_loc * head_dim,), (heads_loc * head_dim,)).reshape(heads_loc, head_dim)
    g_b_1 = lax.dynamic_slice(early[7:7 + ffn // width].reshape(ffn), (me * ffn_loc,), (ffn_loc,))

    return (x_out, g_x.astype(BF), g_y, jnp.concatenate([late[:2], early[:3], late[2:3]], axis=0), g_w_qkv, g_b_qkv.astype(BF), g_w_o.reshape(heads_loc, head_dim, width), early[3].astype(BF), g_w_q.reshape(heads_loc, head_dim, width).transpose(2, 0, 1), g_b_q.astype(BF), g_w_kv, g_b_kv.astype(BF), g_w_co.reshape(heads_loc, head_dim, width), early[5].astype(BF), g_w_1, g_b_1.astype(BF), g_w_2, early[6].astype(BF))


def solution(mesh):
    mesh = jax.sharding.Mesh(mesh.devices.reshape(-1, 2, 2, 2), ('dp',) + TP)
    token_spec = P('dp', TP, None)
    group_rows = ('dp',) + TP
    in_specs = (token_spec, token_spec, P('dp', None), P('dp'), P(None, None), P(None, TP, None), P(TP, None), P(TP, None, None), P(None), P(None, TP, None), P(TP, None), P(None, TP, None), P(TP, None), P(TP, None, None), P(None), P(None, TP), P(TP), P(TP, None), P(None), token_spec)
    out_specs = (token_spec, token_spec, token_spec, P('dp', None), P('dp', TP, None), P(group_rows, None), P(group_rows, None, None), P('dp'), P('dp', TP, None), P(group_rows, None), P('dp', TP, None), P(group_rows, None), P(group_rows, None, None), P('dp'), P('dp', TP), P(group_rows), P(group_rows, None), P('dp'))

    def step(*args):
        return device_block(*args)

    step = jax.shard_map(step, mesh=mesh, in_specs=in_specs, out_specs=out_specs, check_vma=False)
    return step
```

```python
import functools
import math

import jax
import jax.numpy as jnp
from jax import lax
from jax.experimental import pallas as pl
from jax.experimental.pallas import tpu as pltpu
from jax.sharding import PartitionSpec as P


LN_EPS = 1e-6
MASK_FILL = -1e30
N_DEV = 8
TP = ('y', 'x', 'c')
ROW = ('x', 'c')
UNROLL = 1
LOG2E = math.log2(math.e)
BF = jnp.bfloat16
F32 = jnp.float32


def product(form, lhs, rhs):
    return jnp.einsum(form, lhs, rhs, preferred_element_type=F32)


def layer_norm(tensor):
    tensor = tensor.astype(F32)
    centered = tensor - jnp.mean(tensor, axis=-1, keepdims=True)
    inv_std = lax.rsqrt(jnp.mean(centered * centered, axis=-1, keepdims=True) + LN_EPS)
    return centered * inv_std, inv_std


def layer_norm_back(normed, inv_std, g_normed):
    mean_g = jnp.mean(g_normed, axis=-1, keepdims=True)
    mean_gn = jnp.mean(g_normed * normed, axis=-1, keepdims=True)
    return inv_std * (g_normed - mean_g - normed * mean_gn)


def gelu_tanh(tensor):
    return jax.nn.gelu(tensor, approximate=True)


def dot00(lhs, rhs):
    return lax.dot_general(lhs, rhs, (((0,), (0,)), ((), ())), preferred_element_type=F32)


def dot10(lhs, rhs):
    return lax.dot_general(lhs, rhs, (((1,), (0,)), ((), ())), preferred_element_type=F32)


def dot11(lhs, rhs):
    return lax.dot_general(lhs, rhs, (((1,), (1,)), ((), ())), preferred_element_type=F32)


def my_index():
    return lax.axis_index('y') * 4 + lax.axis_index('x') * 2 + lax.axis_index('c')


def device(index):
    return {'y': index // 4, 'x': (index // 2) % 2, 'c': index % 2}


def barrier_signal(me):
    barrier = pltpu.get_barrier_semaphore()
    for k in range(1, N_DEV):
        pl.semaphore_signal(barrier, inc=1, device_id=device(me ^ k), device_id_type=pl.DeviceIdType.MESH)


def barrier_wait():
    pl.semaphore_wait(pltpu.get_barrier_semaphore(), N_DEV - 1)


def block_copy(src, dst, send_sem, recv_sem, peer, k):
    if k == 0:
        return pltpu.make_async_copy(src, dst, recv_sem)
    return pltpu.make_async_remote_copy(src_ref=src, dst_ref=dst, send_sem=send_sem, recv_sem=recv_sem, device_id=device(peer), device_id_type=pl.DeviceIdType.MESH)


def start_all(copies):
    for copy in copies:
        copy.start()


def wait_all(copies):
    for copy in copies:
        copy.wait()


def block_at(index, blk):
    return pl.ds(pl.multiple_of(index * blk, blk), blk)


def attn_fwd_kernel(scale, blk, heads, qkv_ref, kv_ref, o_ref, lse_ref, tok_ref, kv_out, o_scr, send, recv, kv_send, kv_recv):
    i = pl.program_id(0)
    last = pl.num_programs(0) - 1
    tokens = o_ref.shape[2]
    factor = scale * LOG2E
    me = my_index()

    def o_copies(step):
        return [block_copy(o_scr.at[step, :, block_at(me ^ k, blk)], tok_ref.at[step // heads, me * heads + step % heads], send.at[step, k], recv.at[step, k], me ^ k, k) for k in range(N_DEV)]

    kv_copies = [block_copy(kv_ref, kv_out.at[me], kv_send.at[k], kv_recv.at[k], me ^ k, k) for k in range(N_DEV)]

    @pl.when(i == 0)
    def _():
        barrier_signal(me)

    def step(j, carry):
        cols = block_at(j, blk)
        s = dot00(qkv_ref[0, 1], qkv_ref[0, 0, :, cols])
        top = jnp.max(s, axis=0, keepdims=True) * factor
        p = jnp.exp2(s * factor - top)
        total = jnp.sum(p, axis=0, keepdims=True)
        o = dot10(qkv_ref[0, 2], p.astype(BF))
        o_scr[i, :, cols] = (o / total).astype(BF)
        lse_ref[0, :, cols] = top + jnp.log2(total)
        return carry

    lax.fori_loop(0, tokens // blk, step, 0, unroll=UNROLL)
    o_ref[0] = o_scr[i]

    @pl.when(i == 0)
    def _():
        barrier_wait()
        start_all(kv_copies)

    start_all(o_copies(i))

    @pl.when(i == last)
    def _():
        for n in range(o_scr.shape[0]):
            wait_all(o_copies(n))
        wait_all(kv_copies)


def attn_fwd(qkv, kv, heads, blk):
    steps, _, hd, tokens = qkv.shape
    batch = steps // heads
    hbm = pl.BlockSpec(memory_space=pl.ANY)
    dma = pltpu.SemaphoreType.DMA
    return pl.pallas_call(
        functools.partial(attn_fwd_kernel, hd ** -0.5, blk, heads),
        grid=(steps,),
        in_specs=[pl.BlockSpec((1, 3, hd, tokens), lambda i: (i, 0, 0, 0)), hbm],
        out_specs=[pl.BlockSpec((1, hd, tokens), lambda i: (i, 0, 0)), pl.BlockSpec((1, 1, tokens), lambda i: (i, 0, 0)), hbm, hbm],
        out_shape=[jax.ShapeDtypeStruct((steps, hd, tokens), BF), jax.ShapeDtypeStruct((steps, 1, tokens), F32),
                   jax.ShapeDtypeStruct((batch, N_DEV * heads, hd, blk), BF), jax.ShapeDtypeStruct((N_DEV,) + kv.shape, BF)],
        scratch_shapes=[pltpu.VMEM((steps, hd, tokens), BF), dma((steps, N_DEV)), dma((steps, N_DEV)), dma((N_DEV,)), dma((N_DEV,))],
        cost_estimate=pl.CostEstimate(flops=4 * steps * hd * tokens * tokens, bytes_accessed=steps * hd * tokens * 8, transcendentals=steps * tokens * tokens),
        compiler_params=pltpu.CompilerParams(collective_id=1, has_side_effects=True, vmem_limit_bytes=48 << 20),
        name="attn_fwd",
    )(qkv, kv)


def attn_bwd_kernel(scale, blk, heads, qkv_ref, o_ref, lse_ref, g_ref, *refs):
    rows, (d_ref, tok_ref, early_out, g_scr, d_scr, early_scr, dk_acc, dv_acc, g_send, g_recv, d_send, d_recv, x_send, x_recv) = refs[:-14], refs[-14:]
    i = pl.program_id(0)
    steps = d_scr.shape[0]
    tokens = o_ref.shape[2]
    factor = scale * LOG2E
    me = my_index()

    def g_copies(step):
        return [block_copy(g_ref.at[step // heads, (me ^ k) * heads + step % heads], g_scr.at[step, :, block_at(me, blk)], g_send.at[step, k], g_recv.at[step, k], me ^ k, k) for k in range(N_DEV)]

    def d_copies(step):
        return [block_copy(d_scr.at[step, :, :, block_at(me ^ k, blk)], tok_ref.at[step // heads, me * heads + step % heads], d_send.at[step, k], d_recv.at[step, k], me ^ k, k) for k in range(N_DEV)]

    x_copies = [block_copy(early_scr, early_out.at[me], x_send.at[k], x_recv.at[k], me ^ k, k) for k in range(N_DEV)]

    @pl.when(i == 0)
    def _():
        barrier_signal(me)
        barrier_wait()
        for n in range(steps):
            start_all(g_copies(n))
        early_scr[...] = jnp.zeros_like(early_scr)
        place = 0
        for row in rows:
            early_scr[place:place + row.shape[0], :] = row[...]
            place += row.shape[0]

    wait_all(g_copies(i))
    dk_acc[...] = jnp.zeros_like(dk_acc)
    dv_acc[...] = jnp.zeros_like(dv_acc)

    def step(j, carry):
        cols = block_at(j, blk)
        q = qkv_ref[0, 0, :, cols]
        g = g_scr[i, :, cols]
        delta = jnp.sum(g.astype(F32) * o_ref[0, :, cols].astype(F32), axis=0, keepdims=True)
        s = dot00(qkv_ref[0, 1], q)
        p = jnp.exp2(s * factor - lse_ref[0, :, cols])
        dp = dot00(qkv_ref[0, 2], g)
        ds = (p * (dp - delta)).astype(BF)
        dv_acc[...] += dot11(g, p.astype(BF))
        dk_acc[...] += dot11(q, ds)
        d_scr[i, 0, :, cols] = (dot10(qkv_ref[0, 1], ds) * scale).astype(BF)
        return carry

    lax.fori_loop(0, tokens // blk, step, 0, unroll=UNROLL)
    d_scr[i, 1] = (dk_acc[...] * scale).astype(BF)
    d_scr[i, 2] = dv_acc[...].astype(BF)
    d_ref[0] = d_scr[i]
    start_all(d_copies(i))

    @pl.when(i == 0)
    def _():
        start_all(x_copies)

    @pl.when(i == steps - 1)
    def _():
        for n in range(steps):
            wait_all(d_copies(n))
        wait_all(x_copies)


def attn_bwd(qkv, o, lse, g, early, heads, blk):
    steps, _, hd, tokens = qkv.shape
    batch = steps // heads
    hbm = pl.BlockSpec(memory_space=pl.ANY)
    dma = pltpu.SemaphoreType.DMA
    row = lambda i: (i, 0, 0)
    return pl.pallas_call(
        functools.partial(attn_bwd_kernel, hd ** -0.5, blk, heads),
        grid=(steps,),
        in_specs=[pl.BlockSpec((1, 3, hd, tokens), lambda i: (i, 0, 0, 0)), pl.BlockSpec((1, hd, tokens), row), pl.BlockSpec((1, 1, tokens), row), hbm] + [pl.BlockSpec(part.shape, lambda i: (0, 0)) for part in early],
        out_specs=[pl.BlockSpec((1, 3, hd, tokens), lambda i: (i, 0, 0, 0)), hbm, hbm],
        out_shape=[jax.ShapeDtypeStruct(qkv.shape, BF), jax.ShapeDtypeStruct((batch, N_DEV * heads, 3, hd, blk), BF),
                   jax.ShapeDtypeStruct((N_DEV, 16, early[0].shape[1]), F32)],
        scratch_shapes=[pltpu.VMEM((steps, hd, tokens), BF), pltpu.VMEM(qkv.shape, BF), pltpu.VMEM((16, early[0].shape[1]), F32), pltpu.VMEM((hd, tokens), F32), pltpu.VMEM((hd, tokens), F32),
                        dma((steps, N_DEV)), dma((steps, N_DEV)), dma((steps, N_DEV)), dma((steps, N_DEV)), dma((N_DEV,)), dma((N_DEV,))],
        cost_estimate=pl.CostEstimate(flops=10 * steps * hd * tokens * tokens, bytes_accessed=steps * hd * tokens * 20, transcendentals=steps * tokens * tokens),
        compiler_params=pltpu.CompilerParams(collective_id=2, has_side_effects=True, vmem_limit_bytes=56 << 20),
        name="attn_bwd",
    )(qkv, o, lse, g, *early)


def qkv_kernel(w_ref, b_ref, h_ref, out_ref):
    out_ref[0] = (dot11(w_ref[...], h_ref[0]) + b_ref[...]).astype(BF)


def qkv_project(w, bias, first, batch, blk):
    rows, width = w.shape
    return pl.pallas_call(
        qkv_kernel,
        grid=(batch, N_DEV),
        in_specs=[pl.BlockSpec((rows, width), lambda b, j: (0, 0)), pl.BlockSpec((rows, 1), lambda b, j: (0, 0)), pl.BlockSpec((1, blk, width), lambda b, j: (j, b, 0))],
        out_specs=pl.BlockSpec((1, rows, blk), lambda b, j: (b, 0, j)),
        out_shape=jax.ShapeDtypeStruct((batch, rows, N_DEV * blk), BF),
        cost_estimate=pl.CostEstimate(flops=2 * rows * width * batch * N_DEV * blk, bytes_accessed=2 * batch * N_DEV * blk * (rows + width), transcendentals=0),
        compiler_params=pltpu.CompilerParams(vmem_limit_bytes=24 << 20),
        name="qkv_project",
    )(w, bias, first)


def qkv_grad_kernel(g_ref, h_ref, parts, whole, w_ref, b_ref, parts_out, whole_out, w_acc, b_acc, send, recv):
    n = pl.program_id(0)
    me = my_index()
    copies = []
    for k in range(N_DEV):
        copies.append(block_copy(whole, whole_out.at[me], send.at[0, k], recv.at[0, k], me ^ k, k))
        copies.append(block_copy(parts.at[me ^ k], parts_out.at[me], send.at[1, k], recv.at[1, k], me ^ k, k))

    @pl.when(n == 0)
    def _():
        barrier_signal(me)
        w_acc[...] = jnp.zeros_like(w_acc)
        b_acc[...] = jnp.zeros_like(b_acc)

    g = g_ref[0]
    w_acc[...] += dot10(g, h_ref[0])
    b_acc[...] += g.astype(F32)

    @pl.when(n == 0)
    def _():
        barrier_wait()
        start_all(copies)

    @pl.when(n == pl.num_programs(0) - 1)
    def _():
        w_ref[...] = w_acc[...].astype(BF)
        b_ref[...] = jnp.sum(b_acc[...], axis=1, keepdims=True)
        wait_all(copies)


def qkv_grad(g, first, parts, whole, blk):
    batch, rows, tokens = g.shape
    width = first.shape[2]
    hbm = pl.BlockSpec(memory_space=pl.ANY)
    dma = pltpu.SemaphoreType.DMA
    return pl.pallas_call(
        qkv_grad_kernel,
        grid=(batch * N_DEV,),
        in_specs=[pl.BlockSpec((1, rows, blk), lambda n: (n // N_DEV, 0, n % N_DEV)), pl.BlockSpec((1, blk, width), lambda n: (n % N_DEV, n // N_DEV, 0)), hbm, hbm],
        out_specs=[pl.BlockSpec((rows, width), lambda n: (0, 0)), pl.BlockSpec((rows, 1), lambda n: (0, 0)), hbm, hbm],
        out_shape=[jax.ShapeDtypeStruct((rows, width), BF), jax.ShapeDtypeStruct((rows, 1), F32),
                   jax.ShapeDtypeStruct(parts.shape, parts.dtype), jax.ShapeDtypeStruct((N_DEV,) + whole.shape, whole.dtype)],
        scratch_shapes=[pltpu.VMEM((rows, width), F32), pltpu.VMEM((rows, blk), F32), dma((2, N_DEV)), dma((2, N_DEV))],
        cost_estimate=pl.CostEstimate(flops=2 * rows * width * batch * tokens, bytes_accessed=2 * batch * tokens * (rows + width), transcendentals=0),
        compiler_params=pltpu.CompilerParams(collective_id=3, has_side_effects=True, vmem_limit_bytes=24 << 20),
        name="qkv_grad",
    )(g, first, parts, whole)


def cross_fwd_kernel(scale, len_ref, q_ref, kv_ref, c_ref, p_ref):
    heads, slots = q_ref.shape[1], kv_ref.shape[5]
    blk = q_ref.shape[3]
    count = len_ref[pl.program_id(0)]
    ok = lax.broadcasted_iota(jnp.int32, (slots, blk), 0) < count
    for h in range(heads):
        s = dot00(kv_ref[h // 2, 0, h % 2, 0], q_ref[0, h]) * scale
        s = jnp.where(ok, s, MASK_FILL)
        p = jnp.exp(s - jnp.max(s, axis=0, keepdims=True))
        p = (p / jnp.sum(p, axis=0, keepdims=True)).astype(BF)
        p_ref[0, h] = p
        c_ref[0, h] = dot10(kv_ref[h // 2, 0, h % 2, 1], p).astype(BF)


def cross_specs(hd, blk, slots, per):
    q_spec = pl.BlockSpec((1, per, hd, blk), lambda b, i, n: (b, i, 0, 0))
    kv_spec = pl.BlockSpec((per // 2, 1, 2, 2, hd, slots), lambda b, i, n: (i, b, 0, 0, 0, 0))
    p_spec = pl.BlockSpec((1, per, slots, blk), lambda b, i, n: (b, i, 0, 0))
    return q_spec, kv_spec, p_spec


def cross_fwd(lens, q, kv, per=8):
    batch, heads, hd, blk = q.shape
    slots = kv.shape[5]
    q_spec, kv_spec, p_spec = cross_specs(hd, blk, slots, per)
    return pl.pallas_call(
        functools.partial(cross_fwd_kernel, hd ** -0.5),
        grid_spec=pltpu.PrefetchScalarGridSpec(num_scalar_prefetch=1, grid=(batch, heads // per), in_specs=[q_spec, kv_spec], out_specs=[q_spec, p_spec]),
        out_shape=[jax.ShapeDtypeStruct(q.shape, BF), jax.ShapeDtypeStruct((batch, heads, slots, blk), BF)],
        cost_estimate=pl.CostEstimate(flops=4 * batch * heads * hd * blk * slots * 8, bytes_accessed=batch * heads * blk * (hd * 4 + slots * 2), transcendentals=batch * heads * blk * slots),
        compiler_params=pltpu.CompilerParams(vmem_limit_bytes=32 << 20),
        name="cross_fwd",
    )(lens, q, kv)


def cross_bwd_kernel(scale, len_ref, q_ref, kv_ref, p_ref, g_ref, gq_ref, gkv_ref):
    heads = q_ref.shape[1]
    for h in range(heads):
        k, v = kv_ref[h // 2, 0, h % 2, 0], kv_ref[h // 2, 0, h % 2, 1]
        q, g, p = q_ref[0, h], g_ref[0, h], p_ref[0, h]
        dp = dot00(v, g)
        pf = p.astype(F32)
        delta = jnp.sum(dp * pf, axis=0, keepdims=True)
        ds = (pf * (dp - delta) * scale).astype(BF)
        gq_ref[0, h] = dot10(k, ds).astype(BF)
        gkv_ref[h // 2, 0, h % 2, 0] = dot11(q, ds).astype(BF)
        gkv_ref[h // 2, 0, h % 2, 1] = dot11(g, p).astype(BF)


def cross_bwd(lens, q, kv, prob, g, per=8):
    batch, heads, hd, blk = q.shape
    slots = kv.shape[5]
    q_spec, kv_spec, p_spec = cross_specs(hd, blk, slots, per)
    return pl.pallas_call(
        functools.partial(cross_bwd_kernel, hd ** -0.5),
        grid_spec=pltpu.PrefetchScalarGridSpec(num_scalar_prefetch=1, grid=(batch, heads // per), in_specs=[q_spec, kv_spec, p_spec, q_spec], out_specs=[q_spec, kv_spec]),
        out_shape=[jax.ShapeDtypeStruct(q.shape, BF), jax.ShapeDtypeStruct(kv.shape, BF)],
        cost_estimate=pl.CostEstimate(flops=8 * batch * heads * hd * blk * slots * 8, bytes_accessed=batch * heads * blk * (hd * 6 + slots * 2), transcendentals=0),
        compiler_params=pltpu.CompilerParams(vmem_limit_bytes=32 << 20),
        name="cross_bwd",
    )(lens, q, kv, prob, g)


def gather_rows(tensor, axes=TP):
    return lax.all_gather(tensor, axes, axis=0, tiled=True)


def scatter_rows(tensor, axes=TP):
    return lax.psum_scatter(tensor.astype(BF), axes, scatter_dimension=0, tiled=True)


def swap(tensor, axis):
    return lax.ppermute(tensor, axis, [(0, 1), (1, 0)])


def swap_y(tensor):
    return swap(tensor, 'y')


def row_reduce(rows):
    grid = rows.reshape(2, 2, -1, rows.shape[1])
    core = lax.axis_index('c')
    other = swap(lax.dynamic_index_in_dim(grid, 1 - core, 1, keepdims=False), 'c')
    return (lax.dynamic_index_in_dim(grid, core, 1, keepdims=False).astype(F32) + other.astype(F32)).astype(BF)


def row_finish(pair):
    place = lax.axis_index('x')
    other = swap(lax.dynamic_index_in_dim(pair, 1 - place, 0, keepdims=False), 'x')
    return (lax.dynamic_index_in_dim(pair, place, 0, keepdims=False).astype(F32) + other.astype(F32)).astype(BF)


def mlp_hidden(h2, w1_half, b1_half):
    hidden = product('btd,fd->btf', h2, w1_half) + b1_half
    gelu_out, gelu_vjp = jax.vjp(gelu_tanh, hidden)
    return gelu_out.astype(BF), gelu_vjp


def mlp_rest(gelu_out, gelu_vjp, g_mlp, w1_half, w2_half, name):
    g_hidden = gelu_vjp(product('btd,fd->btf', g_mlp, w2_half))[0]
    g_b_1 = jnp.sum(g_hidden, axis=(0, 1))
    g_hidden = g_hidden.astype(BF)
    g_h2 = product('btf,fd->btd', g_hidden, w1_half)
    part = product('btf,fd->btd', gelu_out, w2_half)
    part = part if name == 'own' else part.astype(BF)
    return gelu_out, part, g_hidden, g_b_1, g_h2


def device_block(x_loc, y_loc, t_loc, len_loc, mod_table, w_qkv, b_qkv, w_o, b_o, w_q, b_q, w_kv, b_kv, w_co, b_co, w_1, b_1, w_2, b_2, g_loc):
    batch, n_loc, width = x_loc.shape
    heads_loc, head_dim = w_q.shape[1], w_q.shape[2]
    heads = heads_loc * N_DEV
    inner = heads * head_dim
    slots_loc = y_loc.shape[1]
    slots = slots_loc * N_DEV
    slots_pad = 128
    ffn_loc = w_1.shape[1]
    ffn = ffn_loc * N_DEV
    mod_rows = mod_table.astype(F32)[None] + t_loc.astype(F32).reshape(batch, 6, width)
    shift1, scale1, gate1, shift2, scale2, gate2 = [mod_rows[:, row_idx, None, :] for row_idx in range(6)]

    g_x2 = g_loc.astype(F32)
    g_mlp_f = g_x2 * gate2
    g_b_2 = jnp.sum(g_mlp_f, axis=(0, 1))
    g_mlp = g_mlp_f.astype(BF)

    normed1, inv_std1 = layer_norm(x_loc)
    h1 = (normed1 * (1.0 + scale1) + shift1).astype(BF)

    rows_loc = heads_loc * head_dim
    wqkv_t = w_qkv.transpose(1, 2, 0)
    wkv_t = w_kv.transpose(1, 2, 0)
    wq_t = w_q.transpose(1, 2, 0).reshape(rows_loc, width)
    small = jnp.concatenate([b_q.reshape(-1), b_1])
    small = jnp.pad(small, (0, width - small.shape[0]))[None]
    n_rows = batch * n_loc
    n_text = batch * slots_loc
    first = jnp.concatenate([h1.reshape(n_rows, width), y_loc.reshape(n_text, width), small, jnp.zeros((31 - n_text, width), BF)], axis=0)
    first = gather_rows(first[None])
    y_all = first[:, n_rows:n_rows + n_text].reshape(N_DEV, batch, slots_loc, width).transpose(1, 0, 2, 3).reshape(batch, slots, width)
    y_all = jnp.pad(y_all, ((0, 0), (0, slots_pad - slots), (0, 0)))
    small_all = first[:, n_rows + n_text]
    bq_all = small_all[:, :rows_loc].reshape(inner)
    b1_all = small_all[:, rows_loc:rows_loc + ffn_loc]
    b1_half = lax.dynamic_index_in_dim(b1_all.reshape(2, ffn // 2), lax.axis_index('y'), keepdims=False)
    square = jnp.concatenate([w_o.reshape(rows_loc, width), wq_t, w_co.reshape(rows_loc, width)], axis=0)
    square = gather_rows(square[None])
    w1_half = gather_rows(w_1.T, ROW)
    w2_half = gather_rows(w_2, ROW)
    wqkv_all = gather_rows(wqkv_t.reshape(heads_loc * 3 * head_dim, width))

    tokens = N_DEV * n_loc
    qkv_rows = heads_loc * 3 * head_dim
    qkv = qkv_project(wqkv_t.reshape(qkv_rows, width), b_qkv.astype(F32).reshape(qkv_rows, 1), first, batch, n_loc)
    qkv = qkv.reshape(batch * heads_loc, 3, head_dim, tokens)
    kv_t = (product('hed,bsd->bhes', wkv_t, y_all) + b_kv[None, :, :, None]).astype(BF)
    o_heads, lse, o_tok, kv_all = attn_fwd(qkv, kv_t.reshape(batch, heads_loc, 2, head_dim, slots_pad), heads_loc, n_loc)
    o_tok = o_tok.reshape(batch, inner, n_loc)
    square, o_tok, g_mlp = lax.optimization_barrier((square, o_tok, g_mlp))
    g_mlp_far = swap_y(g_mlp)
    wo_all, wq_all, wco_all = [square[:, n * rows_loc:(n + 1) * rows_loc].reshape(inner, width) for n in range(3)]

    attn_total = product('bet,ed->btd', o_tok, wo_all) + b_o
    x1 = (x_loc + gate1 * attn_total).astype(BF)
    q_cross = (product('ed,btd->bet', wq_all, x1) + bq_all[None, :, None]).astype(BF)
    q_cross = q_cross.reshape(batch, heads, head_dim, n_loc)
    cross_val, cross_prob = cross_fwd(len_loc, q_cross, kv_all)
    cross_rows = cross_val.reshape(batch, inner, n_loc)
    x2 = (x1 + (product('bet,ed->btd', cross_rows, wco_all) + b_co)).astype(BF)

    normed2, inv_std2 = layer_norm(x2)
    h2 = (normed2 * (1.0 + scale2) + shift2).astype(BF)
    gelu_own, vjp_own = mlp_hidden(h2, w1_half, b1_half)
    h2_far = swap_y(h2)
    gelu_far, vjp_far = mlp_hidden(h2_far, w1_half, b1_half)
    w2_half, gelu_own, gelu_far = lax.optimization_barrier((w2_half, gelu_own, gelu_far))
    own = mlp_rest(gelu_own, vjp_own, g_mlp, w1_half, w2_half, 'own')
    far = mlp_rest(gelu_far, vjp_far, g_mlp_far, w1_half, w2_half, 'far')
    g_h2_far, gelu_own, g_hid_own = far[4].astype(BF), own[0], own[2]
    g_h2_far = swap_y(g_h2_far)
    pair = lambda near, other: jnp.concatenate([near, other], axis=0)
    p_w_2 = product('btf,btd->fd', pair(gelu_own, far[0]), pair(g_mlp, g_mlp_far)).astype(BF)
    p_w_2 = row_reduce(p_w_2)
    p_w_1 = product('btf,btd->fd', pair(g_hid_own, far[2]), pair(h2, h2_far)).astype(BF)
    p_w_1 = row_reduce(p_w_1)
    part_own, part_far = own[1], far[1]
    g_h2_far, part_own, part_far, _, _ = lax.optimization_barrier((g_h2_far, part_own, part_far, p_w_2, p_w_1))
    g_h2 = own[4] + g_h2_far.astype(F32)
    part_far = swap_y(part_far)
    g_w_2 = row_finish(p_w_2)
    g_w_1 = row_finish(p_w_1).T
    g_b_1 = own[3] + far[3]
    g_shift2 = jnp.sum(g_h2, axis=(0, 1))
    g_scale2 = jnp.sum(g_h2 * normed2, axis=(0, 1))
    g_x2 = g_x2 + layer_norm_back(normed2, inv_std2, g_h2 * (1.0 + scale2))

    g_b_co = jnp.sum(g_x2, axis=(0, 1))
    g_cross = g_x2.astype(BF)
    p_w_co = product('bet,btd->ed', cross_rows, g_cross).astype(BF)
    g_cross_val = product('btd,ed->bet', g_cross, wco_all).astype(BF).reshape(batch, heads, head_dim, n_loc)
    g_cross_val, wqkv_all = lax.optimization_barrier((g_cross_val, wqkv_all))
    g_q, g_kv = cross_bwd(len_loc, q_cross, kv_all, cross_prob, g_cross_val)
    g_kv = scatter_rows(g_kv)
    g_q = g_q.reshape(batch, inner, n_loc)
    g_b_q = jnp.sum(g_q.astype(F32), axis=(0, 2))
    p_w_q = product('bet,btd->ed', g_q, x1).astype(BF)
    g_x1 = g_x2 + product('bet,ed->btd', g_q, wq_all)
    g_gate1 = jnp.sum(g_x1 * attn_total, axis=(0, 1))
    g_attn_f = g_x1 * gate1
    g_b_o = jnp.sum(g_attn_f, axis=(0, 1))
    g_attn = g_attn_f.astype(BF)
    p_w_o = product('bet,btd->ed', o_tok, g_attn).astype(BF)
    g_o = product('btd,ed->bet', g_attn, wo_all).astype(BF).reshape(batch, heads, head_dim, n_loc)
    g_w_co, g_w_q, g_w_o = scatter_rows(p_w_co), scatter_rows(p_w_q), scatter_rows(p_w_o)
    g_o, _, _, _ = lax.optimization_barrier((g_o, p_w_co, p_w_q, p_w_o))
    g_b_1 = jnp.where(lax.axis_index('y') == jnp.arange(2)[:, None], g_b_1[None], 0.0).reshape(ffn // width, width)
    early = [row[None] for row in (g_gate1, g_shift2, g_scale2, g_b_o, g_b_q, g_b_co, g_b_2)] + [g_b_1]
    g_qkv, g_qkv_tok, early = attn_bwd(qkv, o_heads, lse, g_o, early, heads_loc, n_loc)
    g_qkv_tok, part_far = lax.optimization_barrier((g_qkv_tok, part_far))
    g_kv, g_qkv_tok = lax.optimization_barrier((g_kv, g_qkv_tok))
    g_kv = g_kv.astype(F32).reshape(batch, heads_loc, 2 * head_dim, slots_pad)
    g_b_kv = jnp.sum(g_kv, axis=(0, 3))
    g_kv = g_kv.astype(BF)
    g_y = product('bhes,hed->bsd', g_kv, wkv_t)[:, :slots].astype(BF)
    g_y = g_y.reshape(batch, N_DEV, slots_loc, width).transpose(1, 0, 2, 3).reshape(N_DEV, n_text, width)
    g_y = jnp.pad(g_y, ((0, 0), (0, 32 - n_text), (0, 0)))
    g_w_kv = product('bhes,bsd->hed', g_kv, y_all).astype(BF).transpose(2, 0, 1)
    g_h1 = product('bet,ed->btd', g_qkv_tok.reshape(batch, 3 * inner, n_loc), wqkv_all)
    g_x = g_x1 + layer_norm_back(normed1, inv_std1, g_h1 * (1.0 + scale1))
    mlp_total = part_own + part_far.astype(F32) + b_2
    x_out = (x2 + gate2 * mlp_total).astype(BF)
    g_gate2 = jnp.sum(g_loc.astype(F32) * mlp_total, axis=(0, 1))
    late = jnp.stack([jnp.sum(g_h1, axis=(0, 1)), jnp.sum(g_h1 * normed1, axis=(0, 1)), g_gate2])
    late = jnp.pad(late, ((0, 5), (0, 0)))
    g_w_qkv, g_b_qkv, g_y, late = qkv_grad(g_qkv.reshape(batch, qkv_rows, tokens), first, g_y, late, n_loc)
    g_w_qkv = g_w_qkv.reshape(heads_loc, 3 * head_dim, width).transpose(2, 0, 1)
    g_b_qkv = g_b_qkv.reshape(heads_loc, 3 * head_dim)
    g_y = jnp.sum(g_y.astype(F32), axis=0)[:n_text].reshape(batch, slots_loc, width).astype(BF)
    late = jnp.sum(late, axis=0)
    early = jnp.sum(early, axis=0)
    me = my_index()
    g_b_q = lax.dynamic_slice(early[4], (me * heads_loc * head_dim,), (heads_loc * head_dim,)).reshape(heads_loc, head_dim)
    g_b_1 = lax.dynamic_slice(early[7:7 + ffn // width].reshape(ffn), (me * ffn_loc,), (ffn_loc,))

    return (x_out, g_x.astype(BF), g_y, jnp.concatenate([late[:2], early[:3], late[2:3]], axis=0), g_w_qkv, g_b_qkv.astype(BF), g_w_o.reshape(heads_loc, head_dim, width), early[3].astype(BF), g_w_q.reshape(heads_loc, head_dim, width).transpose(2, 0, 1), g_b_q.astype(BF), g_w_kv, g_b_kv.astype(BF), g_w_co.reshape(heads_loc, head_dim, width), early[5].astype(BF), g_w_1, g_b_1.astype(BF), g_w_2, early[6].astype(BF))


def solution(mesh):
    mesh = jax.sharding.Mesh(mesh.devices.reshape(-1, 2, 2, 2), ('dp',) + TP)
    token_spec = P('dp', TP, None)
    group_rows = ('dp',) + TP
    in_specs = (token_spec, token_spec, P('dp', None), P('dp'), P(None, None), P(None, TP, None), P(TP, None), P(TP, None, None), P(None), P(None, TP, None), P(TP, None), P(None, TP, None), P(TP, None), P(TP, None, None), P(None), P(None, TP), P(TP), P(TP, None), P(None), token_spec)
    out_specs = (token_spec, token_spec, token_spec, P('dp', None), P('dp', TP, None), P(group_rows, None), P(group_rows, None, None), P('dp'), P('dp', TP, None), P(group_rows, None), P('dp', TP, None), P(group_rows, None), P(group_rows, None, None), P('dp'), P('dp', TP), P(group_rows), P(group_rows, None), P('dp'))

    def step(*args):
        return device_block(*args)

    step = jax.shard_map(step, mesh=mesh, in_specs=in_specs, out_specs=out_specs, check_vma=False)
    return step
```
